32 devices in a mesh: section: 2 (over x), dp: 4 (over z), mp: 4 (over y, core).
Axes of the slice: x: 2, y: 2, z: 4, core: 2. Of those that a mesh axis runs over, the one named last changes fastest.
Arguments:
- text_feats: bfloat16 [4096, 512], P('dp'), may hold values from -48 to 48
- image_feats: bfloat16 [4096, 512], P(('dp', 'mp')), may hold values from -48 to 48
- logit_scale: float32 [1], replicated, may hold values from 10 to 320
- layer_inputs: bfloat16 [2, 4096, 512], P('section', 'dp'), may hold values from -6 to 6
- w_in: bfloat16 [2, 512, 2048], P('section', None, 'mp'), may hold values from -0.25 to 0.25
- w_out: bfloat16 [2, 2048, 512], P('section', 'mp'), may hold values from -0.125 to 0.125
Outputs:
- image_grad: bfloat16 [4096, 512], P(('dp', 'mp'))
- input_grad: bfloat16 [4096, 512], P('dp', 'section')
- w_in_grad: float32 [2, 512, 2048], P('section', 'dp', 'mp')
- w_out_grad_t: float32 [2, 512, 2048], P('section', 'dp', 'mp')
The draws below stay inside these ranges and needn't reach their ends.
All inputs are finite; a program needn't handle non-finite values.
Results may differ from the reference program's by a relative error of at most 0.017.
Values may be sent and summed in bfloat16 or wider, within the bound.
A program may use at most 128 MiB of HBM per device.

```python
import jax
import jax.numpy as jnp
from jax import lax

D = 512
FF = 2048
PAIRS_DEV = 1024
PAIRS = 4096
LAYERS = 2


def joint_feats(key):
    folded = jax.random.fold_in(key, 11)
    key_shared, key_text, key_image, key_scale = jax.random.split(folded, 4)
    shared = jnp.clip(jax.random.normal(key_shared, (PAIRS, D), jnp.float32), -4.0, 4.0)
    text_noise = jnp.clip(jax.random.normal(key_text, (PAIRS, D), jnp.float32), -4.0, 4.0)
    image_noise = jnp.clip(jax.random.normal(key_image, (PAIRS, D), jnp.float32), -4.0, 4.0)
    text_rows = shared + text_noise
    image_rows = shared + image_noise
    return (text_rows, image_rows)


def draw_text_feats(key, part):
    text_rows, image_rows = joint_feats(key)
    return text_rows.astype(jnp.bfloat16)


def draw_image_feats(key, part):
    text_rows, image_rows = joint_feats(key)
    return image_rows.astype(jnp.bfloat16)


def draw_logit_scale(key, part):
    folded = jax.random.fold_in(key, 23)
    return jax.random.uniform(folded, (1,), jnp.float32, 10.0, 30.0)


def block_levels(rng, dims, cuts, smallest, top_value):
    factor_of, own = 1.0, jax.random.fold_in(rng, 6)
    for dim, parts in cuts:
        steps = jnp.exp(jax.random.uniform(jax.random.fold_in(own, dim), (parts,), jnp.float32, smallest / len(cuts), top_value / len(cuts)))
        factor_of = factor_of * jnp.repeat(steps, dims[dim] // parts).reshape([-1 if axis == dim else 1 for axis in range(len(dims))])
    return factor_of


def gaussian(key, extent, deviation, limit, cuts=(), kind=jnp.bfloat16):
    entries = jax.random.normal(key, extent, jnp.float32) * deviation
    if len(cuts) > 0:
        entries = block_levels(key, extent, cuts, -0.22, 0.18) * entries
    return jnp.clip(entries, min=-limit, max=limit).astype(kind)


def setup_inputs(seed: int = 0) -> dict:
    splits = jax.random.split(jax.random.key(seed), 7)
    text_feats = draw_text_feats(jax.random.fold_in(splits[6], 71), 0)
    image_feats = draw_image_feats(jax.random.fold_in(splits[6], 71), 0)
    logit_scale = draw_logit_scale(jax.random.fold_in(splits[6], 71), 0)
    layer_inputs = gaussian(splits[3], (LAYERS, PAIRS, D), 1.0, 6.0, ((0, 2), (1, 4)))
    w_in = gaussian(splits[4], (LAYERS, D, FF), D ** -0.5, 0.25, ((0, 2), (2, 4)))
    w_out = gaussian(splits[5], (LAYERS, FF, D), FF ** -0.5, 0.125, ((0, 2), (1, 4)))
    return {"text_feats": text_feats, "image_feats": image_feats, "logit_scale": logit_scale, "layer_inputs": layer_inputs, "w_in": w_in, "w_out": w_out}


def unit_rows(values):
    wide = values.astype(jnp.float32)
    length = jnp.sqrt(lax.optimization_barrier(jnp.sum(wide * wide, axis=1, keepdims=True)) + 1.0)
    return (wide / length, length)

def unit_backward(unit, length, grad_unit):
    return (grad_unit - unit * lax.optimization_barrier(jnp.sum(unit * grad_unit, axis=1, keepdims=True))) / length

def quick_gelu(values):
    return values * jax.nn.sigmoid(1.702 * values)

def quick_slope(values):
    sigm = jax.nn.sigmoid(1.702 * values)
    return sigm + 1.702 * values * sigm * (1.0 - sigm)

def reference(text_feats, image_feats, logit_scale, layer_inputs, w_in, w_out):
    logit_mult = logit_scale[0]
    text_unit, text_length = unit_rows(text_feats)
    image_unit, image_length = unit_rows(image_feats)
    text_low = text_unit.astype(jnp.bfloat16)
    image_low = image_unit.astype(jnp.bfloat16)
    block_count = PAIRS // PAIRS_DEV
    text_blocks = text_low.reshape(block_count, PAIRS_DEV, D)
    block_ids = jnp.arange(block_count, dtype=jnp.int32)
    column_ids = jnp.arange(PAIRS, dtype=jnp.int32)

    def stats_step(state_pair, text_block):
        column_peak, column_total = state_pair
        scores = logit_mult * jnp.dot(text_block, image_low.T, preferred_element_type=jnp.float32)
        row_peak = lax.optimization_barrier(jnp.max(scores, axis=1))
        row_total = lax.optimization_barrier(jnp.sum(jnp.exp(scores - row_peak[:, None]), axis=1))
        new_peak = jnp.maximum(column_peak, lax.optimization_barrier(jnp.max(scores, axis=0)))
        column_total = column_total * jnp.exp(column_peak - new_peak) + lax.optimization_barrier(jnp.sum(jnp.exp(scores - new_peak[None, :]), axis=0))
        return ((new_peak, column_total), (row_peak, row_total))
    start_pair = (jnp.full((PAIRS,), -1e+30, jnp.float32), jnp.zeros((PAIRS,), jnp.float32))
    (column_peak, column_total), (row_peaks, row_totals) = lax.scan(stats_step, start_pair, text_blocks)

    def grad_step(image_acc, inputs):
        text_block, row_peak, row_total, block_id = inputs
        scores = logit_mult * jnp.dot(text_block, image_low.T, preferred_element_type=jnp.float32)
        text_ids = (block_id * PAIRS_DEV + jnp.arange(PAIRS_DEV, dtype=jnp.int32)).astype(jnp.int32)
        positive = (text_ids[:, None] == column_ids[None, :]).astype(jnp.float32)
        row_prob = jnp.exp(scores - row_peak[:, None]) / row_total[:, None]
        column_prob = jnp.exp(scores - column_peak[None, :]) / column_total[None, :]
        score_grad = (0.5 * (row_prob + column_prob) - positive).astype(jnp.bfloat16)
        text_part = logit_mult * jnp.dot(score_grad, image_low, preferred_element_type=jnp.float32)
        image_acc = image_acc + logit_mult * jnp.dot(score_grad.T, text_block, preferred_element_type=jnp.float32)
        return (image_acc, text_part)
    image_unit_grad, text_parts = lax.scan(grad_step, jnp.zeros((PAIRS, D), jnp.float32), (text_blocks, row_peaks, row_totals, block_ids))
    text_unit_grad = text_parts.reshape(PAIRS, D)
    top_grad = unit_backward(text_unit, text_length, text_unit_grad).astype(jnp.bfloat16)
    image_grad = unit_backward(image_unit, image_length, image_unit_grad).astype(jnp.bfloat16)
    layer_grad = top_grad
    first_grads = []
    second_grads = []
    for layer in reversed(range(LAYERS)):
        inputs_now = layer_inputs[layer]
        pre_act = jnp.dot(inputs_now, w_in[layer], preferred_element_type=jnp.float32)
        activation = quick_gelu(pre_act).astype(jnp.bfloat16)
        back_grad = jnp.dot(layer_grad, w_out[layer].T, preferred_element_type=jnp.float32)
        pre_grad = (back_grad * quick_slope(pre_act)).astype(jnp.bfloat16)
        first_grads.insert(0, jnp.dot(inputs_now.T, pre_grad, preferred_element_type=jnp.float32))
        second_grads.insert(0, jnp.dot(layer_grad.T, activation, preferred_element_type=jnp.float32))
        layer_grad = (layer_grad.astype(jnp.float32) + jnp.dot(pre_grad, w_in[layer].T, preferred_element_type=jnp.float32)).astype(jnp.bfloat16)
    return (image_grad, layer_grad, jnp.stack(first_grads), jnp.stack(second_grads))
```

```python
import jax
import jax.numpy as jnp
from jax import lax
from jax.experimental import pallas as pl
from jax.experimental.pallas import tpu as pltpu
from jax.sharding import PartitionSpec as P

MESH = pl.DeviceIdType.MESH
F32 = jnp.float32
BF16 = jnp.bfloat16
GELU = 1.702
LANES = 128
PIECES = 4


def unit_rows(values):
    wide = values.astype(F32)
    length = jnp.sqrt(jnp.sum(wide * wide, axis=1, keepdims=True) + 1.0)
    return (wide / length, length)


def unit_backward(unit, length, grad_unit):
    return (grad_unit - unit * jnp.sum(unit * grad_unit, axis=1, keepdims=True)) / length


def dot_nn(a, b):
    return lax.dot_general(a, b, (((1,), (0,)), ((), ())), preferred_element_type=F32)


def dot_nt(a, b):
    return lax.dot_general(a, b, (((1,), (1,)), ((), ())), preferred_element_type=F32)


def dot_tn(a, b):
    return lax.dot_general(a, b, (((0,), (0,)), ((), ())), preferred_element_type=F32)


def tile(index, size):
    return pl.ds(pl.multiple_of(index * size, size), size)


def pick(index, values):
    out = 0
    for k, v in enumerate(values):
        out = out + jnp.where(index == k, v, 0)
    return out


def nearest(count):
    return [sorted((p for p in range(count) if p != i), key=lambda p: (abs(p - i), p)) for i in range(count)]


def make_kernel(n_sec, n_dp, n_mp):
    cores = 2 if n_mp % 2 == 0 else 1
    chips = n_mp // cores

    def kernel(
        text_in, image_in, scale_ref, hidden_in, w_in, w_out,
        image_out, input_out, first_out, second_out,
        text, image, hidden,
        text_low, cols, scores, sgrad, row_max, row_lse, row_st, row_rx, col_st, col_rx,
        wi_all, wo_all, slope_own, slope_all, act_all, pre_all,
        a_tx, a_rx, b_tx, b_rx, c_tx, c_rx, t_acc, g_all, g_new,
        w_tx, w_rx, i_tx, i_rx,
        ld, gat_s, gat_r, cs_s, cs_r, rs_s, rs_r, wi_s, wi_r, wo_s, wo_r,
        a_s, a_r, b_s, b_r, c_s, c_r, g_s, g_r, x_s, x_r, in_s, in_r, ix_s, ix_r,
        w_s, w_r, im_s, im_r, io_s, io_r,
    ):
        s = lax.axis_index("section")
        d = lax.axis_index("dp")
        m = lax.axis_index("mp")
        last = n_sec - 1
        rows, feats = text.shape
        own = image.shape[0]
        half = own // n_sec
        quarter = rows // n_mp
        piece = quarter // PIECES
        hid = slope_all.shape[1]
        share = feats // n_dp
        width = feats // n_sec
        mult = scale_ref[0]
        core = lax.rem(m, cores)
        chip = m // cores

        def copy(src, dst, send, recv, where):
            return pltpu.make_async_remote_copy(
                src_ref=src, dst_ref=dst, send_sem=send, recv_sem=recv,
                device_id=where, device_id_type=MESH,
            )

        def others(mine, count):
            return [lax.rem(mine + k, count) for k in range(1, count)]

        def sources(mine, count):
            return [lax.rem(mine + count - k, count) for k in range(1, count)]

        order = nearest(n_dp)
        near = [pick(d, [order[i][k] for i in range(n_dp)]) for k in range(n_dp - 1)]
        far = near[::-1]

        barrier = pltpu.get_barrier_semaphore()
        plane = [(t, p) for t in [s] + others(s, n_sec) for p in [m] + others(m, n_mp)][1:]
        for t, p in plane:
            pl.semaphore_signal(barrier, inc=1, device_id={"section": t, "mp": p}, device_id_type=MESH)
        for p in near:
            pl.semaphore_signal(barrier, inc=1, device_id={"dp": p}, device_id_type=MESH)

        loads = [
            pltpu.make_async_copy(image_in, image, ld.at[0]),
            pltpu.make_async_copy(w_in, wi_all.at[m], ld.at[1]),
            pltpu.make_async_copy(w_out, wo_all.at[m], ld.at[2]),
            pltpu.make_async_copy(text_in, text, ld.at[3]),
            pltpu.make_async_copy(hidden_in, hidden, ld.at[4]),
        ]
        for c in loads:
            c.start()

        mine_half = tile(s, half)
        loads[0].wait()
        own_unit, _ = unit_rows(image[mine_half, :])
        cols[tile(d, half), :] = own_unit.astype(BF16)
        loads[1].wait()
        loads[2].wait()
        pl.semaphore_wait(barrier, len(plane) + n_dp - 1)

        gathers = []
        for p in far:
            c = copy(cols.at[tile(d, half), :], cols.at[tile(d, half), :], gat_s.at[p], gat_r.at[d], {"dp": p})
            c.start()
            gathers.append(c)

        class Spread:
            def __init__(self, slot, send, recv):
                self.slot, self.send, self.recv = slot, send, recv
                self.sent = []

            def push(self, index, to):
                c = copy(self.slot(index), self.slot(index), self.send.at[len(self.sent)],
                         self.recv.at[index], {"mp": to})
                c.start()
                self.sent.append(c)

            def arrived(self, index):
                copy(self.slot(index), self.slot(index), self.send.at[0],
                     self.recv.at[index], {"mp": lax.rem(m + 1, n_mp)}).wait_recv()

            def start(self):
                for q in others(chip, chips):
                    self.push(m, q * cores + core)
                for e in others(core, cores):
                    self.push(m, chip * cores + e)

            def relay(self):
                for q in sources(chip, chips):
                    index = q * cores + core
                    self.arrived(index)
                    for e in others(core, cores):
                        self.push(index, chip * cores + e)

            def finish(self):
                for e in sources(core, cores):
                    self.arrived(chip * cores + e)
                    for q in sources(chip, chips):
                        self.arrived(q * cores + e)

            def drain(self):
                for c in self.sent:
                    c.wait_send()

        def cut(ref, n, k):
            size = ref.shape[1] // n
            return lambda j: ref.at[j, k * size : (k + 1) * size, :]

        wi_spread = Spread(cut(wi_all, 1, 0), wi_s, wi_r)
        wo_spread = [Spread(cut(wo_all, 2, k), wo_s.at[k], wo_r.at[k]) for k in range(2)]
        wi_spread.start()

        loads[3].wait()

        @pl.loop(0, n_mp)
        def _(r):
            unit, _ = unit_rows(text[tile(r, quarter), :])
            text_low[tile(r, quarter), :] = unit.astype(BF16)

        row_max[...] = jnp.full(row_max.shape, -1e30, F32)

        def block_scores(p):
            block = cols[tile(p, half), :]
            peak = jnp.full((1, half), -1e30, F32)
            for r in range(n_mp):
                part = pl.ds(r * quarter, quarter)
                value = mult * dot_nt(text_low[part, :], block)
                scores[part, tile(p, half)] = value
                best = row_max[part, :]
                for k in range(0, half, LANES):
                    best = jnp.maximum(best, value[:, k : k + LANES])
                row_max[part, :] = best
                peak = jnp.maximum(peak, jnp.max(value, axis=0, keepdims=True))
            acc = jnp.zeros((1, half), F32)
            for r in range(n_mp):
                value = scores[pl.ds(r * quarter, quarter), tile(p, half)]
                acc = acc + jnp.sum(jnp.exp(value - peak), axis=0, keepdims=True)
            col_st[pl.ds(p, 1), :] = peak
            col_st[pl.ds(n_dp + p, 1), :] = acc

        block_scores(d)

        def gelu_terms(pre):
            sigm = 1.0 / (1.0 + jnp.exp(-GELU * pre))
            return pre * sigm, sigm + GELU * pre * sigm * (1.0 - sigm)

        loads[4].wait()

        @pl.loop(0, n_mp)
        def _(r):
            act, slope = gelu_terms(dot_nn(hidden[tile(r, quarter), :], wi_all[m]))
            act_all[tile(r, quarter), :] = act.astype(BF16)
            slope_all[tile(r, quarter), :] = slope

        @pl.loop(0, n_dp - 1)
        def _(k):
            p = near[0]
            for i in range(1, n_dp - 1):
                p = jnp.where(k == i, near[i], p)
            copy(cols.at[tile(p, half), :], cols.at[tile(p, half), :], gat_s.at[p], gat_r.at[p], {"dp": p}).wait_recv()
            block_scores(p)

        col_rx[d] = col_st[...]
        col_sent = []
        for p in far:
            c = copy(col_st, col_rx.at[d], cs_s.at[p], cs_r.at[d], {"dp": p})
            c.start()
            col_sent.append(c)

        for r in range(n_mp):
            part = pl.ds(r * quarter, quarter)
            peak = jnp.max(row_max[part, :], axis=1, keepdims=True)
            acc = jnp.zeros((quarter, LANES), F32)
            for k in range(0, n_dp * half, LANES):
                acc = acc + jnp.exp(scores[part, k : k + LANES] - peak)
            acc = jnp.sum(acc, axis=1, keepdims=True)
            wide_peak = jnp.broadcast_to(peak, (quarter, LANES)).T
            wide_sum = jnp.broadcast_to(acc, (quarter, LANES)).T
            row_st[r : r + 1, :] = wide_peak[0:1, :]
            row_st[n_mp + r : n_mp + r + 1, :] = wide_sum[0:1, :]

        here = s * n_mp + m
        row_rx[here] = row_st[...]
        row_sent = []
        for k, (t, p) in enumerate(plane):
            c = copy(row_st, row_rx.at[here], rs_s.at[k], rs_r.at[here], {"section": t, "mp": p})
            c.start()
            row_sent.append(c)

        wo_spread[0].start()

        def merge(rx, count, n):
            peak = rx[0, 0:n, :]
            for k in range(1, count):
                peak = jnp.maximum(peak, rx[k, 0:n, :])
            acc = jnp.zeros(peak.shape, F32)
            for k in range(count):
                acc = acc + rx[k, n : 2 * n, :] * jnp.exp(rx[k, 0:n, :] - peak)
            return peak + jnp.log(acc)

        for p in near:
            copy(col_st, col_rx.at[p], cs_s.at[p], cs_r.at[p], {"dp": p}).wait_recv()
        col_lse = merge(col_rx, n_dp, n_dp)
        for t, p in plane:
            copy(row_st, row_rx.at[t * n_mp + p], rs_s.at[0], rs_r.at[t * n_mp + p],
                 {"section": t, "mp": p}).wait_recv()
        merged = merge(row_rx, n_sec * n_mp, n_mp)
        for r in range(n_mp):
            row_lse[r] = jnp.broadcast_to(merged[r : r + 1, :], (LANES, quarter)).T

        def score_rows(r):
            line = row_lse[r]
            for p in range(n_dp):
                for k in range(0, half, LANES):
                    at = pl.ds(p * half + k, LANES)
                    value = scores[tile(r, quarter), at]
                    both = jnp.exp(value - line) + jnp.exp(value - col_lse[p : p + 1, k : k + LANES])
                    sgrad[tile(r, quarter), at] = (0.5 * both).astype(BF16)

        def score_diagonal():
            line = row_lse[m]
            text_id = lax.broadcasted_iota(jnp.int32, (quarter, LANES), 0)
            lse = col_lse[0:1, :]
            for p in range(1, n_dp):
                lse = jnp.where(d == p, col_lse[p : p + 1, :], lse)
            for k in range(0, half, LANES):
                at = pl.ds(pl.multiple_of(d * half + k, LANES), LANES)
                value = scores[tile(m, quarter), at]
                both = jnp.exp(value - line) + jnp.exp(value - lse[:, k : k + LANES])
                image_id = lax.broadcasted_iota(jnp.int32, (quarter, LANES), 1) + (s * half + k)
                out = 0.5 * both - jnp.where(text_id == image_id, 1.0, 0.0)
                sgrad[tile(m, quarter), at] = out.astype(BF16)

        def text_part(r):
            return dot_nn(sgrad[tile(r, quarter), :], cols[...])

        def rows_of(k):
            return tile(k, piece)

        a_sent, b_sent = [], []

        def for_sibling(q):
            for e in others(core, cores):
                r = q * cores + e
                score_rows(r)
                a_tx[q] = text_part(r).astype(BF16)
                c = copy(a_tx.at[q], a_rx.at[q], a_s.at[q], a_r.at[q], {"mp": chip * cores + e})
                c.start()
                a_sent.append(c)

        def from_sibling(q):
            for e in others(core, cores):
                copy(a_tx.at[q], a_rx.at[q], a_s.at[q], a_r.at[q], {"mp": chip * cores + e}).wait_recv()
                t_acc[...] += a_rx[q].astype(F32)

        for q in others(chip, chips):
            for_sibling(q)
            score_rows(q * cores + core)
            t_acc[...] = text_part(q * cores + core)
            from_sibling(q)
            b_tx[q] = t_acc[...].astype(BF16)
            for k in range(PIECES):
                c = copy(b_tx.at[q, rows_of(k), :], b_rx.at[chip, rows_of(k), :], b_s.at[q, k], b_r.at[chip, k],
                         {"mp": q * cores + core})
                c.start()
                b_sent.append(c)
        wo_spread[1].start()
        for_sibling(chip)
        score_rows(m)
        score_diagonal()
        t_acc[...] = text_part(m)

        def image_part(p):
            return dot_tn(sgrad[:, tile(p, half)], text_low[...])

        image_sent = []
        for p in far:
            i_tx[p] = image_part(p).astype(BF16)
            c = copy(i_tx.at[p], i_rx.at[d], im_s.at[p], im_r.at[d], {"dp": p})
            c.start()
            image_sent.append(c)
        i_tx[d] = image_part(d).astype(BF16)

        from_sibling(chip)
        wi_spread.relay()
        wi_spread.finish()
        mine = tile(m, quarter)

        @pl.loop(0, n_mp)
        def _(j):
            _, slope = gelu_terms(dot_nn(hidden[mine, :], wi_all[j]))
            slope_own[j] = slope

        wo_spread[0].relay()

        def gather_sum(k):
            total = t_acc[rows_of(k), :]
            for q in sources(chip, chips):
                copy(b_tx.at[q, rows_of(k), :], b_rx.at[q, rows_of(k), :], b_s.at[q, k], b_r.at[q, k],
                     {"mp": q * cores + core}).wait_recv()
                total = total + b_rx[q, rows_of(k), :].astype(F32)
            return total

        def to_last(k):
            return copy(c_tx.at[rows_of(k), :], c_rx.at[s, rows_of(k), :], c_s.at[k], c_r.at[s, k],
                        {"section": last})

        def to_below(k):
            return copy(g_new.at[rows_of(k), :], g_all.at[m, rows_of(k), :], x_s.at[k], x_r.at[k],
                        {"section": s - 1})

        @pl.when(s != last)
        def _():
            @pl.loop(0, PIECES)
            def _(k):
                c_tx[rows_of(k), :] = gather_sum(k).astype(BF16)
                to_last(k).start()

        wo_spread[1].relay()
        for spread in wo_spread:
            spread.finish()

        def g_copy(k, index, to, sem):
            slot = g_all.at[index, rows_of(k), :]
            return copy(slot, slot, g_s.at[sem, k], g_r.at[index, k], {"mp": to})

        def g_pushes():
            out = [(m, q * cores + core) for q in others(chip, chips)]
            out += [(m, chip * cores + e) for e in others(core, cores)]
            for q in sources(chip, chips):
                out += [(q * cores + core, chip * cores + e) for e in others(core, cores)]
            return out

        pushes = g_pushes()
        first_pushes = chips - 1 + cores - 1

        @pl.loop(0, PIECES)
        def _(k):
            at = tile(m * PIECES + k, piece)

            @pl.when(s == last)
            def _():
                total = gather_sum(k)
                for t in range(last):
                    copy(c_tx.at[rows_of(k), :], c_rx.at[t, rows_of(k), :], c_s.at[k], c_r.at[t, k],
                         {"section": t}).wait_recv()
                    total = total + c_rx[t, rows_of(k), :].astype(F32)
                unit, length = unit_rows(text[at, :])
                g_all[m, rows_of(k), :] = unit_backward(unit, length, mult * total).astype(BF16)

            @pl.when(s != last)
            def _():
                copy(g_new.at[rows_of(k), :], g_all.at[m, rows_of(k), :], x_s.at[k], x_r.at[k],
                     {"section": s + 1}).wait_recv()

            for i, (index, to) in enumerate(pushes[:first_pushes]):
                g_copy(k, index, to, i).start()

            g = g_all[m, rows_of(k), :]
            acc = g.astype(F32)
            for j in range(n_mp):
                grad = (dot_nt(g, wo_all[j]) * slope_own[j, rows_of(k), :]).astype(BF16)
                acc = acc + dot_nt(grad, wi_all[j])
            g_new[rows_of(k), :] = acc.astype(BF16)

            @pl.when(s > 0)
            def _():
                to_below(k).start()

        for k in range(PIECES):
            for q in sources(chip, chips):
                index = q * cores + core
                g_copy(k, index, lax.rem(m + 1, n_mp), 0).wait_recv()
            for i, (index, to) in enumerate(pushes[first_pushes:]):
                g_copy(k, index, to, first_pushes + i).start()

        def slab(k):
            return input_out.at[tile(k, quarter), :]

        def final(t):
            return copy(g_new.at[:, t * width : (t + 1) * width], slab(m), ix_s.at[t], ix_r,
                        {"section": t})

        @pl.when(s == 0)
        def _():
            for t in range(1, n_sec):
                final(t).start()
            input_out[mine, :] = g_new[:, 0:width]

        for k in range(PIECES):
            for e in sources(core, cores):
                for q in [chip] + sources(chip, chips):
                    index = q * cores + e
                    g_copy(k, index, lax.rem(m + 1, n_mp), 0).wait_recv()

        weight_sent = []

        def send_weights(which, grad):
            for p in range(n_dp):
                w_tx[p, which] = grad[p * share : (p + 1) * share, :].astype(BF16)
            for p in far:
                c = copy(w_tx.at[p, which], w_rx.at[d, which], w_s.at[which, p],
                         w_r.at[which, d], {"dp": p})
                c.start()
                weight_sent.append(c)

        send_weights(1, dot_tn(g_all[...].reshape(rows, feats), act_all[...]))

        @pl.loop(0, n_mp)
        def _(r):
            back = dot_nt(g_all[r], wo_all[m])
            pre_all[tile(r, quarter), :] = (back * slope_all[tile(r, quarter), :]).astype(BF16)

        send_weights(0, dot_tn(hidden[...], pre_all[...]))

        in_spread = Spread(slab, in_s, in_r)

        @pl.when(s != 0)
        def _():
            copy(g_new.at[:, 0:width], slab(m), ix_s.at[0], ix_r, {"section": 0}).wait_recv()

        in_spread.start()

        total = i_tx[d].astype(F32)
        for p in near:
            copy(i_tx.at[p], i_rx.at[p], im_s.at[p], im_r.at[p], {"dp": p}).wait_recv()
            total = total + i_rx[p].astype(F32)
        unit, length = unit_rows(image[mine_half, :])
        image_out[mine_half, :] = unit_backward(unit, length, mult * total).astype(BF16)
        out_sent = []
        for t in others(s, n_sec):
            c = copy(image_out.at[mine_half, :], image_out.at[mine_half, :],
                     io_s.at[t], io_r.at[s], {"section": t})
            c.start()
            out_sent.append(c)

        in_spread.relay()
        in_spread.finish()

        for t in sources(s, n_sec):
            part = image_out.at[tile(t, half), :]
            copy(part, part, io_s.at[t], io_r.at[t], {"section": t}).wait_recv()

        for c in gathers + col_sent + row_sent + a_sent + b_sent + image_sent + out_sent:
            c.wait_send()
        for spread in [wi_spread, in_spread] + wo_spread:
            spread.drain()
        for k in range(PIECES):
            for i, (index, to) in enumerate(pushes):
                g_copy(k, index, to, i).wait_send()

        @pl.when(s != last)
        def _():
            for k in range(PIECES):
                to_last(k).wait_send()

        @pl.when(s > 0)
        def _():
            for k in range(PIECES):
                to_below(k).wait_send()

        @pl.when(s == 0)
        def _():
            for t in range(1, n_sec):
                final(t).wait_send()

        for which, out in ((1, second_out), (0, first_out)):
            total = w_tx[d, which].astype(F32)
            for p in near:
                copy(w_tx.at[p, which], w_rx.at[p, which], w_s.at[which, p],
                     w_r.at[which, p], {"dp": p}).wait_recv()
                total = total + w_rx[p, which].astype(F32)
            out[...] = total
        for c in weight_sent:
            c.wait_send()

    return kernel


def store(image, inputs, first, second, image_out, input_out, first_out, second_out, sems):
    copies = [
        pltpu.make_async_copy(image, image_out, sems.at[0]),
        pltpu.make_async_copy(inputs, input_out, sems.at[1]),
        pltpu.make_async_copy(first, first_out.at[0], sems.at[2]),
        pltpu.make_async_copy(second, second_out.at[0], sems.at[3]),
    ]
    for c in copies:
        c.start()
    for c in copies:
        c.wait()


def solution(mesh):
    n_sec, n_dp, n_mp = mesh.shape["section"], mesh.shape["dp"], mesh.shape["mp"]

    def body(text, image, scale, hidden, w_in, w_out):
        rows, feats = text.shape
        own = image.shape[0]
        hid = w_in.shape[2]
        quarter, half, share = rows // n_mp, own // n_sec, feats // n_dp
        columns = half * n_dp
        cores = 2 if n_mp % 2 == 0 else 1
        chips = n_mp // cores
        dma = pltpu.SemaphoreType.DMA
        vmem = pl.BlockSpec(memory_space=pltpu.VMEM)
        hbm = pl.BlockSpec(memory_space=pl.ANY)
        out = pl.pallas_call(
            make_kernel(n_sec, n_dp, n_mp),
            out_shape=(
                jax.ShapeDtypeStruct((own, feats), BF16),
                jax.ShapeDtypeStruct((rows, feats // n_sec), BF16),
                jax.ShapeDtypeStruct((share, hid), F32),
                jax.ShapeDtypeStruct((share, hid), F32),
            ),
            in_specs=[hbm, hbm, pl.BlockSpec(memory_space=pltpu.SMEM), hbm, hbm, hbm],
            out_specs=(vmem,) * 4,
            scratch_shapes=[
                pltpu.VMEM((rows, feats), BF16),
                pltpu.VMEM((own, feats), BF16),
                pltpu.VMEM((rows, feats), BF16),
                pltpu.VMEM((rows, feats), BF16),
                pltpu.VMEM((columns, feats), BF16),
                pltpu.VMEM((rows, columns), F32),
                pltpu.VMEM((rows, columns), BF16),
                pltpu.VMEM((rows, LANES), F32),
                pltpu.VMEM((n_mp, quarter, LANES), F32),
                pltpu.VMEM((2 * n_mp, quarter), F32),
                pltpu.VMEM((n_sec * n_mp, 2 * n_mp, quarter), F32),
                pltpu.VMEM((2 * n_dp, half), F32),
                pltpu.VMEM((n_dp, 2 * n_dp, half), F32),
                pltpu.VMEM((n_mp, feats, hid), BF16),
                pltpu.VMEM((n_mp, hid, feats), BF16),
                pltpu.VMEM((n_mp, quarter, hid), F32),
                pltpu.VMEM((rows, hid), F32),
                pltpu.VMEM((rows, hid), BF16),
                pltpu.VMEM((rows, hid), BF16),
                pltpu.VMEM((chips, quarter, feats), BF16),
                pltpu.VMEM((chips, quarter, feats), BF16),
                pltpu.VMEM((chips, quarter, feats), BF16),
                pltpu.VMEM((chips, quarter, feats), BF16),
                pltpu.VMEM((quarter, feats), BF16),
                pltpu.VMEM((n_sec, quarter, feats), BF16),
                pltpu.VMEM((quarter, feats), F32),
                pltpu.VMEM((n_mp, quarter, feats), BF16),
                pltpu.VMEM((quarter, feats), BF16),
                pltpu.VMEM((n_dp, 2, share, hid), BF16),
                pltpu.VMEM((n_dp, 2, share, hid), BF16),
                pltpu.VMEM((n_dp, half, feats), BF16),
                pltpu.VMEM((n_dp, half, feats), BF16),
                dma((5,)),
                dma((n_dp,)), dma((n_dp,)),
                dma((n_dp,)), dma((n_dp,)),
                dma((n_sec * n_mp,)), dma((n_sec * n_mp,)),
                dma((2 * n_mp,)), dma((n_mp,)),
                dma((2, 2 * n_mp)), dma((2, n_mp)),
                dma((chips,)), dma((chips,)),
                dma((chips, PIECES)), dma((chips, PIECES)),
                dma((PIECES,)), dma((n_sec, PIECES)),
                dma((2 * n_mp, PIECES)), dma((n_mp, PIECES)),
                dma((PIECES,)), dma((PIECES,)),
                dma((2 * n_mp,)), dma((n_mp,)),
                dma((n_sec,)), dma,
                dma((2, n_dp)), dma((2, n_dp)),
                dma((n_dp,)), dma((n_dp,)),
                dma((n_sec,)), dma((n_sec,)),
            ],
            compiler_params=pltpu.CompilerParams(
                collective_id=0, has_side_effects=True, vmem_limit_bytes=63000000
            ),
        )(text, image, scale, hidden[0], w_in[0], w_out[0])
        return tuple(
            pl.pallas_call(
                store,
                out_shape=(
                    jax.ShapeDtypeStruct((own, feats), BF16),
                    jax.ShapeDtypeStruct((rows, feats // n_sec), BF16),
                    jax.ShapeDtypeStruct((1, share, hid), F32),
                    jax.ShapeDtypeStruct((1, share, hid), F32),
                ),
                in_specs=[vmem] * 4,
                out_specs=(hbm,) * 4,
                scratch_shapes=[dma((4,))],
                compiler_params=pltpu.CompilerParams(has_side_effects=True),
            )(*out)
        )

    return jax.shard_map(
        body,
        mesh=mesh,
        in_specs=(
            P("dp", None),
            P(("dp", "mp"), None),
            P(),
            P("section", "dp", None),
            P("section", None, "mp"),
            P("section", "mp", None),
        ),
        out_specs=(
            P(("dp", "mp"), None),
            P("dp", "section"),
            P("section", "dp", "mp"),
            P("section", "dp", "mp"),
        ),
        check_vma=False,
    )
```

```python
import jax
import jax.numpy as jnp
from jax import lax
from jax.experimental import pallas as pl
from jax.experimental.pallas import tpu as pltpu
from jax.sharding import PartitionSpec as P

MESH = pl.DeviceIdType.MESH
F32 = jnp.float32
BF16 = jnp.bfloat16
GELU = 1.702
LANES = 128
PIECES = 4


def unit_rows(values):
    wide = values.astype(F32)
    length = jnp.sqrt(jnp.sum(wide * wide, axis=1, keepdims=True) + 1.0)
    return (wide / length, length)


def unit_backward(unit, length, grad_unit):
    return (grad_unit - unit * jnp.sum(unit * grad_unit, axis=1, keepdims=True)) / length


def dot_nn(a, b):
    return lax.dot_general(a, b, (((1,), (0,)), ((), ())), preferred_element_type=F32)


def dot_nt(a, b):
    return lax.dot_general(a, b, (((1,), (1,)), ((), ())), preferred_element_type=F32)


def dot_tn(a, b):
    return lax.dot_general(a, b, (((0,), (0,)), ((), ())), preferred_element_type=F32)


def tile(index, size):
    return pl.ds(pl.multiple_of(index * size, size), size)


def pick(index, values):
    out = 0
    for k, v in enumerate(values):
        out = out + jnp.where(index == k, v, 0)
    return out


def nearest(count):
    return [sorted((p for p in range(count) if p != i), key=lambda p: (abs(p - i), p)) for i in range(count)]


def make_kernel(n_sec, n_dp, n_mp):
    cores = 2 if n_mp % 2 == 0 else 1
    chips = n_mp // cores

    def kernel(
        text_in, image_in, scale_ref, hidden_in, w_in, w_out,
        image_out, input_out, first_out, second_out,
        text, image, hidden,
        text_low, cols, scores, sgrad, row_max, row_lse, row_st, row_rx, col_st, col_rx,
        raw_in, raw_out, wi_all, wo_all, slope_own, slope_all, act_all, pre_all,
        a_tx, a_rx, b_tx, b_rx, c_tx, c_rx, t_acc, g_all, g_new,
        w_tx, w_rx, w_via, i_tx, i_rx,
        ld, gat_s, gat_r, cs_s, cs_r, rs_s, rs_r, wi_s, wi_r,
        yo_s, yo_r, so_s, so_r, zo_s, zo_r, fo_s, fo_r,
        a_s, a_r, b_s, b_r, c_s, c_r, g_s, g_r, x_s, x_r, in_s, in_r, ix_s, ix_r,
        w_s, w_r, v_s, v_r, im_s, im_r, io_s, io_r,
    ):
        s = lax.axis_index("section")
        d = lax.axis_index("dp")
        m = lax.axis_index("mp")
        last = n_sec - 1
        rows, feats = text.shape
        own = image.shape[0]
        half = own // n_sec
        quarter = rows // n_mp
        piece = quarter // PIECES
        hid = slope_all.shape[1]
        share = feats // n_dp
        width = feats // n_sec
        mult = scale_ref[0]
        core = lax.rem(m, cores)
        chip = m // cores

        def copy(src, dst, send, recv, where):
            return pltpu.make_async_remote_copy(
                src_ref=src, dst_ref=dst, send_sem=send, recv_sem=recv,
                device_id=where, device_id_type=MESH,
            )

        def others(mine, count):
            return [lax.rem(mine + k, count) for k in range(1, count)]

        def sources(mine, count):
            return [lax.rem(mine + count - k, count) for k in range(1, count)]

        order = nearest(n_dp)
        near = [pick(d, [order[i][k] for i in range(n_dp)]) for k in range(n_dp - 1)]
        far = near[::-1]

        barrier = pltpu.get_barrier_semaphore()
        plane = [(t, p) for t in [s] + others(s, n_sec) for p in [m] + others(m, n_mp)][1:]
        for t, p in plane:
            pl.semaphore_signal(barrier, inc=1, device_id={"section": t, "mp": p}, device_id_type=MESH)
        for p in near:
            pl.semaphore_signal(barrier, inc=1, device_id={"dp": p}, device_id_type=MESH)

        loads = [
            pltpu.make_async_copy(image_in, image, ld.at[0]),
            pltpu.make_async_copy(w_in, raw_in, ld.at[1]),
            pltpu.make_async_copy(w_out, raw_out, ld.at[2]),
            pltpu.make_async_copy(text_in, text, ld.at[3]),
            pltpu.make_async_copy(hidden_in, hidden, ld.at[4]),
        ]
        for c in loads:
            c.start()

        mine_half = tile(s, half)
        loads[0].wait()
        own_unit, _ = unit_rows(image[mine_half, :])
        cols[tile(d, half), :] = own_unit.astype(BF16)
        pl.semaphore_wait(barrier, len(plane) + n_dp - 1)

        gathers = []
        for p in far:
            c = copy(cols.at[tile(d, half), :], cols.at[tile(d, half), :], gat_s.at[p], gat_r.at[d], {"dp": p})
            c.start()
            gathers.append(c)

        class Spread:
            def __init__(self, slot, send, recv):
                self.slot, self.send, self.recv = slot, send, recv
                self.sent = []

            def push(self, index, to):
                c = copy(self.slot(index), self.slot(index), self.send.at[len(self.sent)],
                         self.recv.at[index], {"mp": to})
                c.start()
                self.sent.append(c)

            def arrived(self, index):
                copy(self.slot(index), self.slot(index), self.send.at[0],
                     self.recv.at[index], {"mp": lax.rem(m + 1, n_mp)}).wait_recv()

            def start(self):
                for q in others(chip, chips):
                    self.push(m, q * cores + core)
                for e in others(core, cores):
                    self.push(m, chip * cores + e)

            def relay(self):
                for q in sources(chip, chips):
                    index = q * cores + core
                    self.arrived(index)
                    for e in others(core, cores):
                        self.push(index, chip * cores + e)

            def finish(self):
                for e in sources(core, cores):
                    self.arrived(chip * cores + e)
                    for q in sources(chip, chips):
                        self.arrived(q * cores + e)

            def drain(self):
                for c in self.sent:
                    c.wait_send()

        pairs = 2 if n_dp % 2 == 0 else 1
        side = lax.rem(d, pairs)
        depth = feats // pairs

        def wo_part(index, k):
            return wo_all.at[index, tile(k, depth), :]

        loads[2].wait()
        wo_all[m] = raw_out[...].T
        wo_sent = []

        def wo_push(ref, send, recv, to):
            c = copy(ref, ref, send, recv, to)
            c.start()
            wo_sent.append(c)

        for q in others(chip, chips):
            wo_push(wo_part(m, side), yo_s.at[q], yo_r.at[m], {"mp": q * cores + core})
        for e in others(core, cores):
            wo_push(wo_all.at[m], so_s.at[e], so_r.at[m], {"mp": chip * cores + e})

        loads[1].wait()
        wi_all[m] = raw_in[...].T

        def wi_spread_of(k):
            return Spread(lambda j: wi_all.at[j, pl.ds(k * (hid // 2), hid // 2), :], wi_s.at[k], wi_r.at[k])

        wi_spread = [wi_spread_of(k) for k in range(2)]
        wi_spread[0].start()

        def wo_across():
            for q in sources(chip, chips):
                index = q * cores + core
                copy(wo_part(index, side), wo_part(index, side), yo_s.at[q], yo_r.at[index],
                     {"mp": index}).wait_recv()
                if pairs == 2:
                    wo_push(wo_part(index, side), zo_s.at[q], zo_r.at[index], {"dp": d + 1 - 2 * side})
                for e in others(core, cores):
                    wo_push(wo_part(index, side), fo_s.at[q, 0], fo_r.at[index, 0], {"mp": chip * cores + e})

        def wo_along():
            for q in sources(chip, chips):
                index = q * cores + core
                if pairs == 2:
                    copy(wo_part(index, 1 - side), wo_part(index, 1 - side), zo_s.at[q], zo_r.at[index],
                         {"dp": d + 1 - 2 * side}).wait_recv()
                    for e in others(core, cores):
                        wo_push(wo_part(index, 1 - side), fo_s.at[q, 1], fo_r.at[index, 1],
                                {"mp": chip * cores + e})

        def wo_finish():
            for e in sources(core, cores):
                index = chip * cores + e
                copy(wo_all.at[index], wo_all.at[index], so_s.at[e], so_r.at[index], {"mp": index}).wait_recv()
                for q in sources(chip, chips):
                    index = q * cores + e
                    for k in range(pairs):
                        at = wo_part(index, side if k == 0 else 1 - side)
                        copy(at, at, fo_s.at[q, k], fo_r.at[index, k], {"mp": chip * cores + e}).wait_recv()

        loads[3].wait()

        @pl.loop(0, n_mp)
        def _(r):
            unit, _ = unit_rows(text[tile(r, quarter), :])
            text_low[tile(r, quarter), :] = unit.astype(BF16)

        row_max[...] = jnp.full(row_max.shape, -1e30, F32)

        def block_scores(p):
            block = cols[tile(p, half), :]
            peak = jnp.full((1, half), -1e30, F32)
            for r in range(n_mp):
                part = pl.ds(r * quarter, quarter)
                value = mult * dot_nt(text_low[part, :], block)
                scores[part, tile(p, half)] = value
                best = row_max[part, :]
                for k in range(0, half, LANES):
                    best = jnp.maximum(best, value[:, k : k + LANES])
                row_max[part, :] = best
                peak = jnp.maximum(peak, jnp.max(value, axis=0, keepdims=True))
            acc = jnp.zeros((1, half), F32)
            for r in range(n_mp):
                value = scores[pl.ds(r * quarter, quarter), tile(p, half)]
                acc = acc + jnp.sum(jnp.exp(value - peak), axis=0, keepdims=True)
            col_st[pl.ds(p, 1), :] = peak
            col_st[pl.ds(n_dp + p, 1), :] = acc

        block_scores(d)

        def gelu_terms(pre):
            sigm = 1.0 / (1.0 + jnp.exp(-GELU * pre))
            return pre * sigm, sigm + GELU * pre * sigm * (1.0 - sigm)

        loads[4].wait()

        @pl.loop(0, n_mp)
        def _(r):
            act, slope = gelu_terms(dot_nn(hidden[tile(r, quarter), :], raw_in[...]))
            act_all[tile(r, quarter), :] = act.astype(BF16)
            slope_all[tile(r, quarter), :] = slope

        @pl.loop(0, n_dp - 1)
        def _(k):
            p = near[0]
            for i in range(1, n_dp - 1):
                p = jnp.where(k == i, near[i], p)
            copy(cols.at[tile(p, half), :], cols.at[tile(p, half), :], gat_s.at[p], gat_r.at[p], {"dp": p}).wait_recv()
            block_scores(p)

        col_rx[d] = col_st[...]
        col_sent = []
        for p in far:
            c = copy(col_st, col_rx.at[d], cs_s.at[p], cs_r.at[d], {"dp": p})
            c.start()
            col_sent.append(c)

        wo_across()

        for r in range(n_mp):
            part = pl.ds(r * quarter, quarter)
            peak = jnp.max(row_max[part, :], axis=1, keepdims=True)
            acc = jnp.zeros((quarter, LANES), F32)
            for k in range(0, n_dp * half, LANES):
                acc = acc + jnp.exp(scores[part, k : k + LANES] - peak)
            acc = jnp.sum(acc, axis=1, keepdims=True)
            wide_peak = jnp.broadcast_to(peak, (quarter, LANES)).T
            wide_sum = jnp.broadcast_to(acc, (quarter, LANES)).T
            row_st[r : r + 1, :] = wide_peak[0:1, :]
            row_st[n_mp + r : n_mp + r + 1, :] = wide_sum[0:1, :]

        here = s * n_mp + m
        row_rx[here] = row_st[...]
        row_sent = []
        for k, (t, p) in enumerate(plane):
            c = copy(row_st, row_rx.at[here], rs_s.at[k], rs_r.at[here], {"section": t, "mp": p})
            c.start()
            row_sent.append(c)

        wi_spread[1].start()
        wi_spread[0].relay()

        def merge(rx, count, n):
            peak = rx[0, 0:n, :]
            for k in range(1, count):
                peak = jnp.maximum(peak, rx[k, 0:n, :])
            acc = jnp.zeros(peak.shape, F32)
            for k in range(count):
                acc = acc + rx[k, n : 2 * n, :] * jnp.exp(rx[k, 0:n, :] - peak)
            return peak + jnp.log(acc)

        for p in near:
            copy(col_st, col_rx.at[p], cs_s.at[p], cs_r.at[p], {"dp": p}).wait_recv()
        col_lse = merge(col_rx, n_dp, n_dp)
        for t, p in plane:
            copy(row_st, row_rx.at[t * n_mp + p], rs_s.at[0], rs_r.at[t * n_mp + p],
                 {"section": t, "mp": p}).wait_recv()
        merged = merge(row_rx, n_sec * n_mp, n_mp)
        for r in range(n_mp):
            row_lse[r] = jnp.broadcast_to(merged[r : r + 1, :], (LANES, quarter)).T

        def score_rows(r):
            line = row_lse[r]
            for p in range(n_dp):
                for k in range(0, half, LANES):
                    at = pl.ds(p * half + k, LANES)
                    value = scores[tile(r, quarter), at]
                    both = jnp.exp(value - line) + jnp.exp(value - col_lse[p : p + 1, k : k + LANES])
                    sgrad[tile(r, quarter), at] = (0.5 * both).astype(BF16)

        def score_diagonal():
            line = row_lse[m]
            text_id = lax.broadcasted_iota(jnp.int32, (quarter, LANES), 0)
            lse = col_lse[0:1, :]
            for p in range(1, n_dp):
                lse = jnp.where(d == p, col_lse[p : p + 1, :], lse)
            for k in range(0, half, LANES):
                at = pl.ds(pl.multiple_of(d * half + k, LANES), LANES)
                value = scores[tile(m, quarter), at]
                both = jnp.exp(value - line) + jnp.exp(value - lse[:, k : k + LANES])
                image_id = lax.broadcasted_iota(jnp.int32, (quarter, LANES), 1) + (s * half + k)
                out = 0.5 * both - jnp.where(text_id == image_id, 1.0, 0.0)
                sgrad[tile(m, quarter), at] = out.astype(BF16)

        def text_part(r):
            return dot_nn(sgrad[tile(r, quarter), :], cols[...])

        def rows_of(k):
            return tile(k, piece)

        a_sent, b_sent = [], []

        def for_sibling(q):
            for e in others(core, cores):
                r = q * cores + e
                score_rows(r)
                a_tx[q] = text_part(r).astype(BF16)
                c = copy(a_tx.at[q], a_rx.at[q], a_s.at[q], a_r.at[q], {"mp": chip * cores + e})
                c.start()
                a_sent.append(c)

        def from_sibling(q):
            for e in others(core, cores):
                copy(a_tx.at[q], a_rx.at[q], a_s.at[q], a_r.at[q], {"mp": chip * cores + e}).wait_recv()
                t_acc[...] += a_rx[q].astype(F32)

        for q in others(chip, chips):
            for_sibling(q)
            score_rows(q * cores + core)
            t_acc[...] = text_part(q * cores + core)
            from_sibling(q)
            b_tx[q] = t_acc[...].astype(BF16)
            for k in range(PIECES):
                c = copy(b_tx.at[q, rows_of(k), :], b_rx.at[chip, rows_of(k), :], b_s.at[q, k], b_r.at[chip, k],
                         {"mp": q * cores + core})
                c.start()
                b_sent.append(c)
        for_sibling(chip)
        score_rows(m)
        score_diagonal()
        t_acc[...] = text_part(m)

        def image_part(p):
            return dot_tn(sgrad[:, tile(p, half)], text_low[...])

        image_sent = []
        for p in far:
            i_tx[p] = image_part(p).astype(BF16)
            c = copy(i_tx.at[p], i_rx.at[d], im_s.at[p], im_r.at[d], {"dp": p})
            c.start()
            image_sent.append(c)
        i_tx[d] = image_part(d).astype(BF16)

        from_sibling(chip)
        mine = tile(m, quarter)
        wi_spread[1].relay()
        wo_along()

        def own_slope(j):
            _, slope = gelu_terms(dot_nt(hidden[mine, :], wi_all[j]))
            slope_own[j] = slope

        own_slope(m)
        for spread in wi_spread:
            spread.finish()

        @pl.loop(1, n_mp)
        def _(k):
            own_slope(lax.rem(m + k, n_mp))

        wo_finish()

        def gather_sum(k):
            total = t_acc[rows_of(k), :]
            for q in sources(chip, chips):
                copy(b_tx.at[q, rows_of(k), :], b_rx.at[q, rows_of(k), :], b_s.at[q, k], b_r.at[q, k],
                     {"mp": q * cores + core}).wait_recv()
                total = total + b_rx[q, rows_of(k), :].astype(F32)
            return total

        def to_last(k):
            return copy(c_tx.at[rows_of(k), :], c_rx.at[s, rows_of(k), :], c_s.at[k], c_r.at[s, k],
                        {"section": last})

        def to_below(k):
            return copy(g_new.at[rows_of(k), :], g_all.at[m, rows_of(k), :], x_s.at[k], x_r.at[k],
                        {"section": s - 1})

        @pl.when(s != last)
        def _():
            @pl.loop(0, PIECES)
            def _(k):
                c_tx[rows_of(k), :] = gather_sum(k).astype(BF16)
                to_last(k).start()


        def g_copy(k, index, to, sem):
            slot = g_all.at[index, rows_of(k), :]
            return copy(slot, slot, g_s.at[sem, k], g_r.at[index, k], {"mp": to})

        def g_pushes():
            out = [(m, q * cores + core) for q in others(chip, chips)]
            out += [(m, chip * cores + e) for e in others(core, cores)]
            for q in sources(chip, chips):
                out += [(q * cores + core, chip * cores + e) for e in others(core, cores)]
            return out

        pushes = g_pushes()
        first_pushes = chips - 1 + cores - 1

        @pl.loop(0, PIECES)
        def _(k):
            at = tile(m * PIECES + k, piece)

            @pl.when(s == last)
            def _():
                total = gather_sum(k)
                for t in range(last):
                    copy(c_tx.at[rows_of(k), :], c_rx.at[t, rows_of(k), :], c_s.at[k], c_r.at[t, k],
                         {"section": t}).wait_recv()
                    total = total + c_rx[t, rows_of(k), :].astype(F32)
                unit, length = unit_rows(text[at, :])
                g_all[m, rows_of(k), :] = unit_backward(unit, length, mult * total).astype(BF16)

            @pl.when(s != last)
            def _():
                copy(g_new.at[rows_of(k), :], g_all.at[m, rows_of(k), :], x_s.at[k], x_r.at[k],
                     {"section": s + 1}).wait_recv()

            for i, (index, to) in enumerate(pushes[:first_pushes]):
                g_copy(k, index, to, i).start()

            g = g_all[m, rows_of(k), :]
            acc = g.astype(F32)
            for j in range(n_mp):
                grad = (dot_nn(g, wo_all[j]) * slope_own[j, rows_of(k), :]).astype(BF16)
                acc = acc + dot_nn(grad, wi_all[j])
            g_new[rows_of(k), :] = acc.astype(BF16)

            @pl.when(s > 0)
            def _():
                to_below(k).start()

        for k in range(PIECES):
            for q in sources(chip, chips):
                index = q * cores + core
                g_copy(k, index, lax.rem(m + 1, n_mp), 0).wait_recv()
            for i, (index, to) in enumerate(pushes[first_pushes:]):
                g_copy(k, index, to, first_pushes + i).start()

        def slab(k):
            return input_out.at[tile(k, quarter), :]

        def final(t):
            return copy(g_new.at[:, t * width : (t + 1) * width], slab(m), ix_s.at[t], ix_r,
                        {"section": t})

        @pl.when(s == 0)
        def _():
            for t in range(1, n_sec):
                final(t).start()
            input_out[mine, :] = g_new[:, 0:width]

        for k in range(PIECES):
            for e in sources(core, cores):
                for q in [chip] + sources(chip, chips):
                    index = q * cores + e
                    g_copy(k, index, lax.rem(m + 1, n_mp), 0).wait_recv()

        weight_sent = []
        via_hub = n_dp == 4
        end = (d == 0) | (d == n_dp - 1)
        hub = jnp.where(d == 0, 1, n_dp - 2)

        def to_dp(which, p):
            return copy(w_tx.at[p, which], w_rx.at[d, which], w_s.at[which, p], w_r.at[which, d], {"dp": p})

        def to_hub(which):
            return copy(w_tx.at[far[0], which], w_via.at[which], v_s.at[which], v_r.at[which], {"dp": hub})

        def send_weights(which, grad):
            for p in range(n_dp):
                w_tx[p, which] = grad[p * share : (p + 1) * share, :].astype(BF16)
            if via_hub:
                @pl.when(end)
                def _():
                    to_hub(which).start()
            for p in far[1:] if via_hub else far:
                c = to_dp(which, p)
                c.start()
                weight_sent.append(c)

        def pass_on(which):
            if via_hub:
                @pl.when(jnp.logical_not(end))
                def _():
                    to_hub(which).wait_recv()
                    both = w_tx[far[0], which].astype(F32) + w_via[which].astype(F32)
                    w_tx[far[0], which] = both.astype(BF16)
                    to_dp(which, far[0]).start()

        send_weights(1, dot_tn(g_all[...].reshape(rows, feats), act_all[...]))

        @pl.loop(0, n_mp)
        def _(r):
            back = dot_nn(g_all[r], wo_all[m])
            pre_all[tile(r, quarter), :] = (back * slope_all[tile(r, quarter), :]).astype(BF16)

        send_weights(0, dot_tn(hidden[...], pre_all[...]))

        pass_on(1)
        in_spread = Spread(slab, in_s, in_r)

        @pl.when(s != 0)
        def _():
            copy(g_new.at[:, 0:width], slab(m), ix_s.at[0], ix_r, {"section": 0}).wait_recv()

        in_spread.start()

        total = i_tx[d].astype(F32)
        for p in near:
            copy(i_tx.at[p], i_rx.at[p], im_s.at[p], im_r.at[p], {"dp": p}).wait_recv()
            total = total + i_rx[p].astype(F32)
        unit, length = unit_rows(image[mine_half, :])
        image_out[mine_half, :] = unit_backward(unit, length, mult * total).astype(BF16)
        out_sent = []
        for t in others(s, n_sec):
            c = copy(image_out.at[mine_half, :], image_out.at[mine_half, :],
                     io_s.at[t], io_r.at[s], {"section": t})
            c.start()
            out_sent.append(c)

        in_spread.relay()
        pass_on(0)
        in_spread.finish()

        for t in sources(s, n_sec):
            part = image_out.at[tile(t, half), :]
            copy(part, part, io_s.at[t], io_r.at[t], {"section": t}).wait_recv()

        for c in gathers + col_sent + row_sent + a_sent + b_sent + image_sent + out_sent:
            c.wait_send()
        for spread in wi_spread + [in_spread]:
            spread.drain()
        for c in wo_sent:
            c.wait_send()
        for k in range(PIECES):
            for i, (index, to) in enumerate(pushes):
                g_copy(k, index, to, i).wait_send()

        @pl.when(s != last)
        def _():
            for k in range(PIECES):
                to_last(k).wait_send()

        @pl.when(s > 0)
        def _():
            for k in range(PIECES):
                to_below(k).wait_send()

        @pl.when(s == 0)
        def _():
            for t in range(1, n_sec):
                final(t).wait_send()

        for which, out in ((1, second_out), (0, first_out)):
            out[...] = w_tx[d, which].astype(F32)

            def add(p):
                copy(w_tx.at[p, which], w_rx.at[p, which], w_s.at[which, p], w_r.at[which, p],
                     {"dp": p}).wait_recv()
                out[...] += w_rx[p, which].astype(F32)

            for k, p in enumerate(near):
                if via_hub and k == n_dp - 2:
                    pl.when(jnp.logical_not(end))(lambda p=p: add(p))
                else:
                    add(p)
        for c in weight_sent:
            c.wait_send()
        if via_hub:
            for which in range(2):
                @pl.when(end)
                def _():
                    to_hub(which).wait_send()

                @pl.when(jnp.logical_not(end))
                def _():
                    to_dp(which, far[0]).wait_send()

    return kernel


def store(image, inputs, first, second, image_out, input_out, first_out, second_out, sems):
    copies = [
        pltpu.make_async_copy(image, image_out, sems.at[0]),
        pltpu.make_async_copy(inputs, input_out, sems.at[1]),
        pltpu.make_async_copy(first, first_out.at[0], sems.at[2]),
        pltpu.make_async_copy(second, second_out.at[0], sems.at[3]),
    ]
    for c in copies:
        c.start()
    for c in copies:
        c.wait()


def solution(mesh):
    n_sec, n_dp, n_mp = mesh.shape["section"], mesh.shape["dp"], mesh.shape["mp"]

    def body(text, image, scale, hidden, w_in, w_out):
        rows, feats = text.shape
        own = image.shape[0]
        hid = w_in.shape[2]
        quarter, half, share = rows // n_mp, own // n_sec, feats // n_dp
        columns = half * n_dp
        cores = 2 if n_mp % 2 == 0 else 1
        chips = n_mp // cores
        dma = pltpu.SemaphoreType.DMA
        vmem = pl.BlockSpec(memory_space=pltpu.VMEM)
        hbm = pl.BlockSpec(memory_space=pltpu.HBM)
        out = pl.pallas_call(
            make_kernel(n_sec, n_dp, n_mp),
            out_shape=(
                pltpu.VMEM((own, feats), BF16),
                pltpu.VMEM((rows, feats // n_sec), BF16),
                pltpu.VMEM((share, hid), F32),
                pltpu.VMEM((share, hid), F32),
            ),
            in_specs=[hbm, hbm, pl.BlockSpec(memory_space=pltpu.SMEM), hbm, hbm, hbm],
            out_specs=(vmem,) * 4,
            scratch_shapes=[
                pltpu.VMEM((rows, feats), BF16),
                pltpu.VMEM((own, feats), BF16),
                pltpu.VMEM((rows, feats), BF16),
                pltpu.VMEM((rows, feats), BF16),
                pltpu.VMEM((columns, feats), BF16),
                pltpu.VMEM((rows, columns), F32),
                pltpu.VMEM((rows, columns), BF16),
                pltpu.VMEM((rows, LANES), F32),
                pltpu.VMEM((n_mp, quarter, LANES), F32),
                pltpu.VMEM((2 * n_mp, quarter), F32),
                pltpu.VMEM((n_sec * n_mp, 2 * n_mp, quarter), F32),
                pltpu.VMEM((2 * n_dp, half), F32),
                pltpu.VMEM((n_dp, 2 * n_dp, half), F32),
                pltpu.VMEM((feats, hid), BF16),
                pltpu.VMEM((hid, feats), BF16),
                pltpu.VMEM((n_mp, hid, feats), BF16),
                pltpu.VMEM((n_mp, feats, hid), BF16),
                pltpu.VMEM((n_mp, quarter, hid), F32),
                pltpu.VMEM((rows, hid), F32),
                pltpu.VMEM((rows, hid), BF16),
                pltpu.VMEM((rows, hid), BF16),
                pltpu.VMEM((chips, quarter, feats), BF16),
                pltpu.VMEM((chips, quarter, feats), BF16),
                pltpu.VMEM((chips, quarter, feats), BF16),
                pltpu.VMEM((chips, quarter, feats), BF16),
                pltpu.VMEM((quarter, feats), BF16),
                pltpu.VMEM((n_sec, quarter, feats), BF16),
                pltpu.VMEM((quarter, feats), F32),
                pltpu.VMEM((n_mp, quarter, feats), BF16),
                pltpu.VMEM((quarter, feats), BF16),
                pltpu.VMEM((n_dp, 2, share, hid), BF16),
                pltpu.VMEM((n_dp, 2, share, hid), BF16),
                pltpu.VMEM((2, share, hid), BF16),
                pltpu.VMEM((n_dp, half, feats), BF16),
                pltpu.VMEM((n_dp, half, feats), BF16),
                dma((5,)),
                dma((n_dp,)), dma((n_dp,)),
                dma((n_dp,)), dma((n_dp,)),
                dma((n_sec * n_mp,)), dma((n_sec * n_mp,)),
                dma((2, 2 * n_mp)), dma((2, n_mp)),
                dma((chips,)), dma((n_mp,)), dma((cores,)), dma((n_mp,)),
                dma((chips,)), dma((n_mp,)), dma((chips, 2)), dma((n_mp, 2)),
                dma((chips,)), dma((chips,)),
                dma((chips, PIECES)), dma((chips, PIECES)),
                dma((PIECES,)), dma((n_sec, PIECES)),
                dma((2 * n_mp, PIECES)), dma((n_mp, PIECES)),
                dma((PIECES,)), dma((PIECES,)),
                dma((2 * n_mp,)), dma((n_mp,)),
                dma((n_sec,)), dma,
                dma((2, n_dp)), dma((2, n_dp)),
                dma((2,)), dma((2,)),
                dma((n_dp,)), dma((n_dp,)),
                dma((n_sec,)), dma((n_sec,)),
            ],
            compiler_params=pltpu.CompilerParams(
                collective_id=0, has_side_effects=True, vmem_limit_bytes=50000000
            ),
        )(*(pltpu.with_memory_space_constraint(x, pltpu.HBM) for x in (text, image)), scale,
          *(pltpu.with_memory_space_constraint(x[0], pltpu.HBM) for x in (hidden, w_in, w_out)))
        return tuple(
            pl.pallas_call(
                store,
                out_shape=(
                    jax.ShapeDtypeStruct((own, feats), BF16),
                    jax.ShapeDtypeStruct((rows, feats // n_sec), BF16),
                    jax.ShapeDtypeStruct((1, share, hid), F32),
                    jax.ShapeDtypeStruct((1, share, hid), F32),
                ),
                in_specs=[vmem] * 4,
                out_specs=(hbm,) * 4,
                scratch_shapes=[dma((4,))],
                compiler_params=pltpu.CompilerParams(has_side_effects=True),
            )(*(pltpu.with_memory_space_constraint(x, pltpu.VMEM) for x in out))
        )

    return jax.shard_map(
        body,
        mesh=mesh,
        in_specs=(
            P("dp", None),
            P(("dp", "mp"), None),
            P(),
            P("section", "dp", None),
            P("section", None, "mp"),
            P("section", "mp", None),
        ),
        out_specs=(
            P(("dp", "mp"), None),
            P("dp", "section"),
            P("section", "dp", "mp"),
            P("section", "dp", "mp"),
        ),
        check_vma=False,
    )
```

```python
import jax
import jax.numpy as jnp
from jax import lax
from jax.experimental import pallas as pl
from jax.experimental.pallas import tpu as pltpu
from jax.sharding import PartitionSpec as P

MESH = pl.DeviceIdType.MESH
F32 = jnp.float32
BF16 = jnp.bfloat16
GELU = 1.702
LANES = 128
PIECES = 8
GROUP = 2


def unit_rows(values):
    wide = values.astype(F32)
    length = jnp.sqrt(jnp.sum(wide * wide, axis=1, keepdims=True) + 1.0)
    return (wide / length, length)


def unit_backward(unit, length, grad_unit):
    return (grad_unit - unit * jnp.sum(unit * grad_unit, axis=1, keepdims=True)) / length


def dot_nn(a, b):
    return lax.dot_general(a, b, (((1,), (0,)), ((), ())), preferred_element_type=F32)


def dot_nt(a, b):
    return lax.dot_general(a, b, (((1,), (1,)), ((), ())), preferred_element_type=F32)


def dot_tn(a, b):
    return lax.dot_general(a, b, (((0,), (0,)), ((), ())), preferred_element_type=F32)


def tile(index, size):
    return pl.ds(pl.multiple_of(index * size, size), size)


def pick(index, values):
    out = 0
    for k, v in enumerate(values):
        out = out + jnp.where(index == k, v, 0)
    return out


def nearest(count):
    return [sorted((p for p in range(count) if p != i), key=lambda p: (abs(p - i), p)) for i in range(count)]


def make_kernel(n_sec, n_dp, n_mp):
    cores = 2 if n_mp % 2 == 0 else 1
    chips = n_mp // cores

    def kernel(
        text_in, image_in, scale_ref, hidden_in, w_in, w_out,
        image_out, input_out, first_out, second_out,
        text, image, hidden,
        text_low, cols, scores, sgrad, row_max, row_sum, row_lse, row_st, row_rx, col_st, col_rx,
        raw_in, raw_out, wi_all, wo_all, slope_own, slope_all, act_all, pre_all, grad_own,
        a_tx, a_rx, b_tx, b_rx, c_tx, c_rx, t_acc, g_all, g_new,
        w_tx, w_rx, w_via, i_tx, i_rx,
        ld, gat_s, gat_r, cs_s, cs_r, rs_s, rs_r, wi_s, wi_a, wi_i,
        wo_s, yo_r, so_r, zo_r, fo_r, a_s, a_r, b_s, b_r, c_s, c_r, g_s, ga_r, gi_r, x_s, x_r,
        in_s, in_a, in_i, ix_s, ix_r, w_s, w_r, v_r, im_s, im_r, io_s, io_r,
    ):
        s = lax.axis_index("section")
        d = lax.axis_index("dp")
        m = lax.axis_index("mp")
        last = n_sec - 1
        rows, feats = text.shape
        own = image.shape[0]
        half = own // n_sec
        quarter = rows // n_mp
        piece = quarter // PIECES
        hid = slope_all.shape[1]
        share = feats // n_dp
        width = feats // n_sec
        mult = scale_ref[0]
        core = lax.rem(m, cores)
        chip = m // cores

        def copy(src, dst, send, recv, where):
            return pltpu.make_async_remote_copy(
                src_ref=src, dst_ref=dst, send_sem=send, recv_sem=recv,
                device_id=where, device_id_type=MESH,
            )

        def wait_sent(ref, sem):
            pltpu.make_async_copy(ref, ref, sem).wait()

        def others(mine, count):
            return [lax.rem(mine + k, count) for k in range(1, count)]

        def sources(mine, count):
            return [lax.rem(mine + count - k, count) for k in range(1, count)]

        order = nearest(n_dp)
        near = [pick(d, [order[i][k] for i in range(n_dp)]) for k in range(n_dp - 1)]
        far = near[::-1]

        barrier = pltpu.get_barrier_semaphore()
        plane = [(t, p) for t in [s] + others(s, n_sec) for p in [m] + others(m, n_mp)][1:]
        for t, p in plane:
            pl.semaphore_signal(barrier, inc=1, device_id={"section": t, "mp": p}, device_id_type=MESH)
        for p in near:
            pl.semaphore_signal(barrier, inc=1, device_id={"dp": p}, device_id_type=MESH)

        loads = [
            pltpu.make_async_copy(image_in, image, ld.at[0]),
            pltpu.make_async_copy(w_in, raw_in, ld.at[1]),
            pltpu.make_async_copy(w_out, raw_out, ld.at[2]),
            pltpu.make_async_copy(text_in, text, ld.at[3]),
            pltpu.make_async_copy(hidden_in, hidden, ld.at[4]),
        ]
        for c in loads:
            c.start()

        mine_half = tile(s, half)
        loads[0].wait()
        own_unit, _ = unit_rows(image[mine_half, :])
        cols[tile(d, half), :] = own_unit.astype(BF16)
        pl.semaphore_wait(barrier, len(plane) + n_dp - 1)

        for p in far:
            copy(cols.at[tile(d, half), :], cols.at[tile(d, half), :], gat_s, gat_r.at[d], {"dp": p}).start()

        class Spread:
            def __init__(self, slot, send, across, inside):
                self.slot, self.send, self.across, self.inside = slot, send, across, inside

            def push(self, index, recv, to):
                copy(self.slot(index), self.slot(index), self.send, recv, {"mp": to}).start()

            def start(self):
                for q in others(chip, chips):
                    self.push(m, self.across.at[chip], q * cores + core)
                for e in others(core, cores):
                    self.push(m, self.inside.at[chip], chip * cores + e)

            def relay(self):
                for q in sources(chip, chips):
                    index = q * cores + core
                    copy(self.slot(index), self.slot(index), self.send, self.across.at[q], {"mp": index}).wait_recv()
                    for e in others(core, cores):
                        self.push(index, self.inside.at[q], chip * cores + e)

            def finish(self):
                for e in sources(core, cores):
                    for q in range(chips):
                        slot = self.slot(q * cores + e)
                        copy(slot, slot, self.send, self.inside.at[q], {"mp": chip * cores + e}).wait_recv()

        pairs = 2 if n_dp % 2 == 0 else 1
        side = lax.rem(d, pairs)
        depth = feats // pairs

        def wo_part(index, k):
            return wo_all.at[index, tile(k, depth), :]

        loads[2].wait()
        wo_all[m] = raw_out[...].T
        def wo_push(ref, recv, to):
            copy(ref, ref, wo_s, recv, to).start()

        for q in others(chip, chips):
            wo_push(wo_part(m, side), yo_r.at[chip], {"mp": q * cores + core})
        for e in others(core, cores):
            wo_push(wo_all.at[m], so_r, {"mp": chip * cores + e})

        loads[1].wait()
        wi_all[m] = raw_in[...].T

        def wi_spread_of(k):
            return Spread(lambda j: wi_all.at[j, pl.ds(k * (hid // 2), hid // 2), :], wi_s, wi_a.at[k], wi_i.at[k])

        wi_spread = [wi_spread_of(k) for k in range(2)]
        wi_spread[0].start()

        def wo_across():
            for q in sources(chip, chips):
                index = q * cores + core
                at = wo_part(index, side)
                copy(at, at, wo_s, yo_r.at[q], {"mp": index}).wait_recv()
                if pairs == 2:
                    wo_push(at, zo_r.at[q], {"dp": d + 1 - 2 * side})
                for e in others(core, cores):
                    wo_push(at, fo_r.at[q, 0], {"mp": chip * cores + e})

        def wo_along():
            for q in sources(chip, chips):
                at = wo_part(q * cores + core, 1 - side)
                if pairs == 2:
                    copy(at, at, wo_s, zo_r.at[q], {"dp": d + 1 - 2 * side}).wait_recv()
                    for e in others(core, cores):
                        wo_push(at, fo_r.at[q, 1], {"mp": chip * cores + e})

        def wo_finish():
            for e in sources(core, cores):
                to = {"mp": chip * cores + e}
                own_block = wo_all.at[chip * cores + e]
                copy(own_block, own_block, wo_s, so_r, to).wait_recv()
                for q in sources(chip, chips):
                    for k in range(pairs):
                        at = wo_part(q * cores + e, side if k == 0 else 1 - side)
                        copy(at, at, wo_s, fo_r.at[q, k], to).wait_recv()

        loads[3].wait()

        @pl.loop(0, n_mp)
        def _(r):
            unit, _ = unit_rows(text[tile(r, quarter), :])
            text_low[tile(r, quarter), :] = unit.astype(BF16)

        row_max[...] = jnp.full(row_max.shape, -1e30, F32)
        row_sum[...] = jnp.zeros(row_sum.shape, F32)

        def block_scores(p):
            block = cols[tile(p, half), :]
            peak = jnp.full((1, half), -1e30, F32)
            for r in range(n_mp):
                part = pl.ds(r * quarter, quarter)
                value = mult * dot_nt(text_low[part, :], block)
                scores[part, tile(p, half)] = value
                peak = jnp.maximum(peak, jnp.max(value, axis=0, keepdims=True))
            acc = jnp.zeros((1, half), F32)
            for r in range(n_mp):
                value = scores[pl.ds(r * quarter, quarter), tile(p, half)]
                acc = acc + jnp.sum(jnp.exp(value - peak), axis=0, keepdims=True)
            col_st[pl.ds(p, 1), :] = peak
            col_st[pl.ds(n_dp + p, 1), :] = acc

        def block_rows(p):
            for r in range(n_mp):
                part = pl.ds(r * quarter, quarter)
                old = row_max[part, :]
                best = old
                value = [scores[part, pl.ds(pl.multiple_of(p * half + k, LANES), LANES)] for k in range(0, half, LANES)]
                for v in value:
                    best = jnp.maximum(best, v)
                acc = row_sum[part, :] * jnp.exp(old - best)
                for v in value:
                    acc = acc + jnp.exp(v - best)
                row_max[part, :] = best
                row_sum[part, :] = acc

        block_scores(d)
        block_rows(d)

        def gelu_terms(pre):
            sigm = 1.0 / (1.0 + jnp.exp(-GELU * pre))
            return pre * sigm, sigm + GELU * pre * sigm * (1.0 - sigm)

        loads[4].wait()

        @pl.loop(0, n_mp)
        def _(r):
            act, slope = gelu_terms(dot_nn(hidden[tile(r, quarter), :], raw_in[...]))
            act_all[tile(r, quarter), :] = act.astype(BF16)
            slope_all[tile(r, quarter), :] = slope

        @pl.loop(0, n_dp - 1)
        def _(k):
            p = near[0]
            for i in range(1, n_dp - 1):
                p = jnp.where(k == i, near[i], p)
            copy(cols.at[tile(p, half), :], cols.at[tile(p, half), :], gat_s, gat_r.at[p], {"dp": p}).wait_recv()
            block_scores(p)

            @pl.when(k < n_dp - 2)
            def _():
                block_rows(p)

        col_rx[d] = col_st[...]
        for p in far:
            copy(col_st, col_rx.at[d], cs_s, cs_r.at[d], {"dp": p}).start()

        wo_across()
        block_rows(far[0])

        for r in range(n_mp):
            part = pl.ds(r * quarter, quarter)
            peak = jnp.max(row_max[part, :], axis=1, keepdims=True)
            acc = jnp.sum(row_sum[part, :] * jnp.exp(row_max[part, :] - peak), axis=1, keepdims=True)
            wide_peak = jnp.broadcast_to(peak, (quarter, LANES)).T
            wide_sum = jnp.broadcast_to(acc, (quarter, LANES)).T
            row_st[r : r + 1, :] = wide_peak[0:1, :]
            row_st[n_mp + r : n_mp + r + 1, :] = wide_sum[0:1, :]

        here = s * n_mp + m
        row_rx[here] = row_st[...]
        for k, (t, p) in enumerate(plane):
            copy(row_st, row_rx.at[here], rs_s, rs_r.at[here], {"section": t, "mp": p}).start()

        wi_spread[1].start()
        wi_spread[0].relay()

        def merge(rx, count, n):
            peak = rx[0, 0:n, :]
            for k in range(1, count):
                peak = jnp.maximum(peak, rx[k, 0:n, :])
            acc = jnp.zeros(peak.shape, F32)
            for k in range(count):
                acc = acc + rx[k, n : 2 * n, :] * jnp.exp(rx[k, 0:n, :] - peak)
            return peak + jnp.log(acc)

        for p in near:
            copy(col_st, col_rx.at[p], cs_s, cs_r.at[p], {"dp": p}).wait_recv()
        col_lse = merge(col_rx, n_dp, n_dp)
        for t, p in plane:
            copy(row_st, row_rx.at[t * n_mp + p], rs_s, rs_r.at[t * n_mp + p], {"section": t, "mp": p}).wait_recv()
        merged = merge(row_rx, n_sec * n_mp, n_mp)
        for r in range(n_mp):
            row_lse[r] = jnp.broadcast_to(merged[r : r + 1, :], (LANES, quarter)).T

        def score_rows(r):
            line = row_lse[r]
            for p in range(n_dp):
                for k in range(0, half, LANES):
                    at = pl.ds(p * half + k, LANES)
                    value = scores[tile(r, quarter), at]
                    both = jnp.exp(value - line) + jnp.exp(value - col_lse[p : p + 1, k : k + LANES])
                    sgrad[tile(r, quarter), at] = (0.5 * both).astype(BF16)

        def score_diagonal():
            line = row_lse[m]
            text_id = lax.broadcasted_iota(jnp.int32, (quarter, LANES), 0)
            lse = col_lse[0:1, :]
            for p in range(1, n_dp):
                lse = jnp.where(d == p, col_lse[p : p + 1, :], lse)
            for k in range(0, half, LANES):
                at = pl.ds(pl.multiple_of(d * half + k, LANES), LANES)
                value = scores[tile(m, quarter), at]
                both = jnp.exp(value - line) + jnp.exp(value - lse[:, k : k + LANES])
                image_id = lax.broadcasted_iota(jnp.int32, (quarter, LANES), 1) + (s * half + k)
                out = 0.5 * both - jnp.where(text_id == image_id, 1.0, 0.0)
                sgrad[tile(m, quarter), at] = out.astype(BF16)

        def text_part(r):
            return dot_nn(sgrad[tile(r, quarter), :], cols[...])

        def rows_of(k):
            return tile(k, piece)

        def for_sibling(q):
            for e in others(core, cores):
                r = q * cores + e
                score_rows(r)
                a_tx[q] = text_part(r).astype(BF16)
                copy(a_tx.at[q], a_rx.at[q], a_s, a_r.at[q], {"mp": chip * cores + e}).start()

        def from_sibling(q):
            for e in others(core, cores):
                copy(a_tx.at[q], a_rx.at[q], a_s, a_r.at[q], {"mp": chip * cores + e}).wait_recv()
                t_acc[...] += a_rx[q].astype(F32)

        for q in others(chip, chips):
            for_sibling(q)
            score_rows(q * cores + core)
            t_acc[...] = text_part(q * cores + core)
            from_sibling(q)
            b_tx[q] = t_acc[...].astype(BF16)
            for k in range(PIECES):
                copy(b_tx.at[q, rows_of(k), :], b_rx.at[chip, rows_of(k), :], b_s, b_r.at[chip, k],
                     {"mp": q * cores + core}).start()
        for_sibling(chip)
        score_rows(m)
        score_diagonal()
        t_acc[...] = text_part(m)

        def image_part(p):
            return dot_tn(sgrad[:, tile(p, half)], text_low[...])

        for p in far:
            i_tx[p] = image_part(p).astype(BF16)
            copy(i_tx.at[p], i_rx.at[d], im_s, im_r.at[d], {"dp": p}).start()
        i_tx[d] = image_part(d).astype(BF16)

        from_sibling(chip)
        mine = tile(m, quarter)
        wi_spread[1].relay()
        wo_along()

        def gather_sum(k):
            total = t_acc[rows_of(k), :]
            for q in sources(chip, chips):
                copy(b_tx.at[q, rows_of(k), :], b_rx.at[q, rows_of(k), :], b_s, b_r.at[q, k],
                     {"mp": q * cores + core}).wait_recv()
                total = total + b_rx[q, rows_of(k), :].astype(F32)
            return total

        def to_last(k):
            return copy(c_tx.at[rows_of(k), :], c_rx.at[s, rows_of(k), :], c_s, c_r.at[s, k],
                        {"section": last})

        def to_below(k):
            return copy(g_new.at[rows_of(k), :], g_all.at[m, rows_of(k), :], x_s, x_r.at[k],
                        {"section": s - 1})

        @pl.when(s != last)
        def _():
            @pl.loop(0, PIECES)
            def _(k):
                c_tx[rows_of(k), :] = gather_sum(k).astype(BF16)
                to_last(k).start()

        def own_slope(j):
            _, slope = gelu_terms(dot_nt(hidden[mine, :], wi_all[j]))
            slope_own[j] = slope

        own_slope(m)
        for spread in wi_spread:
            spread.finish()

        @pl.loop(1, n_mp)
        def _(k):
            own_slope(lax.rem(m + k, n_mp))

        wo_finish()

        def g_push(k, index, recv, to):
            slot = g_all.at[index, rows_of(k), :]
            copy(slot, slot, g_s, recv, {"mp": to}).start()

        @pl.loop(0, PIECES // GROUP)
        def _(i):
            @pl.loop(i * GROUP, (i + 1) * GROUP)
            def _(k):
                at = tile(m * PIECES + k, piece)

                @pl.when(s == last)
                def _():
                    total = gather_sum(k)
                    for t in range(last):
                        copy(c_tx.at[rows_of(k), :], c_rx.at[t, rows_of(k), :], c_s, c_r.at[t, k],
                             {"section": t}).wait_recv()
                        total = total + c_rx[t, rows_of(k), :].astype(F32)
                    unit, length = unit_rows(text[at, :])
                    g_all[m, rows_of(k), :] = unit_backward(unit, length, mult * total).astype(BF16)

                @pl.when(s != last)
                def _():
                    copy(g_new.at[rows_of(k), :], g_all.at[m, rows_of(k), :], x_s, x_r.at[k],
                         {"section": s + 1}).wait_recv()

                for q in others(chip, chips):
                    g_push(k, m, ga_r.at[chip, k], q * cores + core)

            group = tile(i, GROUP * piece)
            for e in others(core, cores):
                slot = g_all.at[m, group, :]
                copy(slot, slot, g_s, gi_r.at[chip, i], {"mp": chip * cores + e}).start()
            g = g_all[m, group, :]
            for j in range(n_mp):
                back = dot_nn(g, wo_all[j])
                grad_own[:, j * hid : (j + 1) * hid] = (back * slope_own[j, group, :]).astype(BF16)
            acc = dot_nn(grad_own[...], wi_all[...].reshape(n_mp * hid, feats))
            g_new[group, :] = (g.astype(F32) + acc).astype(BF16)

            @pl.when(s > 0)
            def _():
                for k in range(GROUP):
                    to_below(i * GROUP + k).start()

        for i in range(PIECES // GROUP):
            group = pl.ds(i * GROUP * piece, GROUP * piece)
            for q in sources(chip, chips):
                index = q * cores + core
                for k in range(i * GROUP, (i + 1) * GROUP):
                    slot = g_all.at[index, rows_of(k), :]
                    copy(slot, slot, g_s, ga_r.at[q, k], {"mp": index}).wait_recv()
                slot = g_all.at[index, group, :]
                for e in others(core, cores):
                    copy(slot, slot, g_s, gi_r.at[q, i], {"mp": chip * cores + e}).start()

        def slab(k):
            return input_out.at[tile(k, quarter), :]

        def final(t):
            return copy(g_new.at[:, t * width : (t + 1) * width], slab(m), ix_s, ix_r,
                        {"section": t})

        @pl.when(s == 0)
        def _():
            for t in range(1, n_sec):
                final(t).start()
            input_out[mine, :] = g_new[:, 0:width]

        for i in range(PIECES // GROUP):
            for e in sources(core, cores):
                for q in range(chips):
                    slot = g_all.at[q * cores + e, pl.ds(i * GROUP * piece, GROUP * piece), :]
                    copy(slot, slot, g_s, gi_r.at[q, i], {"mp": chip * cores + e}).wait_recv()

        via_hub = n_dp == 4
        mate = d + 1 - 2 * lax.rem(d, 2)
        low = d < n_dp // 2
        end = (d == 0) | (d == n_dp - 1)
        inner = jnp.logical_not(end)
        cross = [jnp.where(low, n_dp - 1, 0), jnp.where(low, n_dp - 2, 1)]

        def weight_grad(which, at):
            if which == 1:
                left = g_all[:, :, at]
                return dot_tn(left.reshape(rows, left.shape[2]), act_all[...]).astype(BF16)
            return dot_tn(hidden[:, at], pre_all[...]).astype(BF16)

        def to_dp(which, p, slot):
            return copy(w_tx.at[p, which], w_rx.at[slot, which], w_s, w_r.at[which, slot], {"dp": p})

        def to_hub(which, k):
            return copy(w_tx.at[cross[k], which], w_via.at[which, k], w_s, v_r.at[which, k], {"dp": mate})

        def send_weights(which):
            if via_hub:
                for k in range(2):
                    w_tx[cross[k], which] = weight_grad(which, tile(cross[k], share))

                    @pl.when(end)
                    def _():
                        to_hub(which, k).start()

                w_tx[mate, which] = weight_grad(which, tile(mate, share))

                @pl.when(inner)
                def _():
                    to_dp(which, mate, 0).start()

                if which == 0:

                    @pl.when(end)
                    def _():
                        to_dp(1, mate, 0).start()
                        to_dp(0, mate, 0).start()

                w_tx[d, which] = weight_grad(which, tile(d, share))
            else:
                grad = weight_grad(which, pl.ds(0, feats))
                for p in range(n_dp):
                    w_tx[p, which] = grad[p * share : (p + 1) * share, :]
                for p in far:
                    to_dp(which, p, d).start()

        def pass_on(which, k):
            if via_hub:

                @pl.when(inner)
                def _():
                    to_hub(which, k).wait_recv()
                    both = w_tx[cross[k], which].astype(F32) + w_via[which, k].astype(F32)
                    w_tx[cross[k], which] = both.astype(BF16)
                    to_dp(which, cross[k], 1).start()

        send_weights(1)

        @pl.loop(0, n_mp)
        def _(r):
            back = dot_nn(g_all[r], wo_all[m])
            pre_all[tile(r, quarter), :] = (back * slope_all[tile(r, quarter), :]).astype(BF16)

        send_weights(0)
        pass_on(1, 0)
        pass_on(1, 1)
        in_spread = Spread(slab, in_s, in_a, in_i)

        @pl.when(s != 0)
        def _():
            copy(g_new.at[:, 0:width], slab(m), ix_s, ix_r, {"section": 0}).wait_recv()

        in_spread.start()

        total = i_tx[d].astype(F32)
        for p in near:
            copy(i_tx.at[p], i_rx.at[p], im_s, im_r.at[p], {"dp": p}).wait_recv()
            total = total + i_rx[p].astype(F32)
        unit, length = unit_rows(image[mine_half, :])
        image_out[mine_half, :] = unit_backward(unit, length, mult * total).astype(BF16)
        for t in others(s, n_sec):
            copy(image_out.at[mine_half, :], image_out.at[mine_half, :], io_s, io_r.at[s], {"section": t}).start()

        pass_on(0, 0)
        in_spread.relay()
        in_spread.finish()
        pass_on(0, 1)

        for t in sources(s, n_sec):
            part = image_out.at[tile(t, half), :]
            copy(part, part, io_s, io_r.at[t], {"section": t}).wait_recv()

        wait_sent(cols.at[pl.ds(0, (n_dp - 1) * half), :], gat_s)
        wait_sent(col_rx.at[pl.ds(0, n_dp - 1)], cs_s)
        wait_sent(row_rx.at[pl.ds(0, n_sec * n_mp - 1)], rs_s)
        wait_sent(wi_all.at[pl.ds(0, n_mp - 1)], wi_s)
        wait_sent(wo_all.at[pl.ds(0, n_mp - 1)], wo_s)
        if cores > 1:
            wait_sent(a_tx, a_s)
        if chips > 1:
            wait_sent(b_tx.at[pl.ds(0, chips - 1)], b_s)
        wait_sent(g_all.at[pl.ds(0, n_mp - 1)], g_s)
        wait_sent(i_tx.at[pl.ds(0, n_dp - 1)], im_s)
        wait_sent(input_out.at[pl.ds(0, (n_mp - 1) * quarter), :], in_s)
        wait_sent(image_out.at[pl.ds(0, (n_sec - 1) * half), :], io_s)

        @pl.when(s != last)
        def _():
            wait_sent(c_tx, c_s)

        @pl.when(s > 0)
        def _():
            wait_sent(g_new, x_s)

        @pl.when(s == 0)
        def _():
            wait_sent(g_new.at[:, pl.ds(0, (n_sec - 1) * width)], ix_s)

        for which, out in ((1, second_out), (0, first_out)):
            out[...] = w_tx[d, which].astype(F32)

            for p in [0, 1] if via_hub else near:
                copy(w_rx.at[p, which], w_rx.at[p, which], w_s, w_r.at[which, p], {"dp": mate}).wait_recv()
                out[...] += w_rx[p, which].astype(F32)
        wait_sent(w_tx.at[pl.ds(0, n_dp - 1)], w_s)

    return kernel


def store(image, inputs, first, second, image_out, input_out, first_out, second_out, sems):
    copies = [
        pltpu.make_async_copy(image, image_out, sems.at[0]),
        pltpu.make_async_copy(inputs, input_out, sems.at[1]),
        pltpu.make_async_copy(first, first_out.at[0], sems.at[2]),
        pltpu.make_async_copy(second, second_out.at[0], sems.at[3]),
    ]
    for c in copies:
        c.start()
    for c in copies:
        c.wait()


def solution(mesh):
    n_sec, n_dp, n_mp = mesh.shape["section"], mesh.shape["dp"], mesh.shape["mp"]

    def body(text, image, scale, hidden, w_in, w_out):
        rows, feats = text.shape
        own = image.shape[0]
        hid = w_in.shape[2]
        quarter, half, share = rows // n_mp, own // n_sec, feats // n_dp
        columns = half * n_dp
        cores = 2 if n_mp % 2 == 0 else 1
        chips = n_mp // cores
        dma = pltpu.SemaphoreType.DMA
        vmem = pl.BlockSpec(memory_space=pltpu.VMEM)
        hbm = pl.BlockSpec(memory_space=pltpu.HBM)
        out = pl.pallas_call(
            make_kernel(n_sec, n_dp, n_mp),
            out_shape=(
                pltpu.VMEM((own, feats), BF16),
                pltpu.VMEM((rows, feats // n_sec), BF16),
                pltpu.VMEM((share, hid), F32),
                pltpu.VMEM((share, hid), F32),
            ),
            in_specs=[hbm, hbm, pl.BlockSpec(memory_space=pltpu.SMEM), hbm, hbm, hbm],
            out_specs=(vmem,) * 4,
            scratch_shapes=[
                pltpu.VMEM((rows, feats), BF16),
                pltpu.VMEM((own, feats), BF16),
                pltpu.VMEM((rows, feats), BF16),
                pltpu.VMEM((rows, feats), BF16),
                pltpu.VMEM((columns, feats), BF16),
                pltpu.VMEM((rows, columns), F32),
                pltpu.VMEM((rows, columns), BF16),
                pltpu.VMEM((rows, LANES), F32),
                pltpu.VMEM((rows, LANES), F32),
                pltpu.VMEM((n_mp, quarter, LANES), F32),
                pltpu.VMEM((2 * n_mp, quarter), F32),
                pltpu.VMEM((n_sec * n_mp, 2 * n_mp, quarter), F32),
                pltpu.VMEM((2 * n_dp, half), F32),
                pltpu.VMEM((n_dp, 2 * n_dp, half), F32),
                pltpu.VMEM((feats, hid), BF16),
                pltpu.VMEM((hid, feats), BF16),
                pltpu.VMEM((n_mp, hid, feats), BF16),
                pltpu.VMEM((n_mp, feats, hid), BF16),
                pltpu.VMEM((n_mp, quarter, hid), F32),
                pltpu.VMEM((rows, hid), F32),
                pltpu.VMEM((rows, hid), BF16),
                pltpu.VMEM((rows, hid), BF16),
                pltpu.VMEM((quarter // PIECES * GROUP, n_mp * hid), BF16),
                pltpu.VMEM((chips, quarter, feats), BF16),
                pltpu.VMEM((chips, quarter, feats), BF16),
                pltpu.VMEM((chips, quarter, feats), BF16),
                pltpu.VMEM((chips, quarter, feats), BF16),
                pltpu.VMEM((quarter, feats), BF16),
                pltpu.VMEM((n_sec, quarter, feats), BF16),
                pltpu.VMEM((quarter, feats), F32),
                pltpu.VMEM((n_mp, quarter, feats), BF16),
                pltpu.VMEM((quarter, feats), BF16),
                pltpu.VMEM((n_dp, 2, share, hid), BF16),
                pltpu.VMEM((n_dp, 2, share, hid), BF16),
                pltpu.VMEM((2, 2, share, hid), BF16),
                pltpu.VMEM((n_dp, half, feats), BF16),
                pltpu.VMEM((n_dp, half, feats), BF16),
                dma((5,)),
                dma, dma((n_dp,)),
                dma, dma((n_dp,)),
                dma, dma((n_sec * n_mp,)),
                dma, dma((2, chips)), dma((2, chips)),
                dma, dma((chips,)), dma, dma((chips,)), dma((chips, 2)),
                dma, dma((chips,)),
                dma, dma((chips, PIECES)),
                dma, dma((n_sec, PIECES)),
                dma, dma((chips, PIECES)), dma((chips, PIECES // GROUP)),
                dma, dma((PIECES,)),
                dma, dma((chips,)), dma((chips,)),
                dma, dma,
                dma, dma((2, 2 if n_dp == 4 else n_dp)), dma((2, 2)),
                dma, dma((n_dp,)),
                dma, dma((n_sec,)),
            ],
            compiler_params=pltpu.CompilerParams(
                collective_id=0, has_side_effects=True, vmem_limit_bytes=50000000
            ),
        )(*(pltpu.with_memory_space_constraint(x, pltpu.HBM) for x in (text, image)), scale,
          *(pltpu.with_memory_space_constraint(x[0], pltpu.HBM) for x in (hidden, w_in, w_out)))
        return tuple(
            pl.pallas_call(
                store,
                out_shape=(
                    jax.ShapeDtypeStruct((own, feats), BF16),
                    jax.ShapeDtypeStruct((rows, feats // n_sec), BF16),
                    jax.ShapeDtypeStruct((1, share, hid), F32),
                    jax.ShapeDtypeStruct((1, share, hid), F32),
                ),
                in_specs=[vmem] * 4,
                out_specs=(hbm,) * 4,
                scratch_shapes=[dma((4,))],
                compiler_params=pltpu.CompilerParams(has_side_effects=True),
            )(*(pltpu.with_memory_space_constraint(x, pltpu.VMEM) for x in out))
        )

    return jax.shard_map(
        body,
        mesh=mesh,
        in_specs=(
            P("dp", None),
            P(("dp", "mp"), None),
            P(),
            P("section", "dp", None),
            P("section", None, "mp"),
            P("section", "mp", None),
        ),
        out_specs=(
            P(("dp", "mp"), None),
            P("dp", "section"),
            P("section", "dp", "mp"),
            P("section", "dp", "mp"),
        ),
        check_vma=False,
    )
```

```python
import jax
import jax.numpy as jnp
from jax import lax
from jax.experimental import pallas as pl
from jax.experimental.pallas import tpu as pltpu
from jax.sharding import PartitionSpec as P

MESH = pl.DeviceIdType.MESH
F32 = jnp.float32
BF16 = jnp.bfloat16
GELU = 1.702
LANES = 128
PIECES = 8
GROUP = 2


def unit_rows(values):
    wide = values.astype(F32)
    length = jnp.sqrt(jnp.sum(wide * wide, axis=1, keepdims=True) + 1.0)
    return (wide / length, length)


def unit_backward(unit, length, grad_unit):
    return (grad_unit - unit * jnp.sum(unit * grad_unit, axis=1, keepdims=True)) / length


def dot_nn(a, b):
    return lax.dot_general(a, b, (((1,), (0,)), ((), ())), preferred_element_type=F32)


def dot_nt(a, b):
    return lax.dot_general(a, b, (((1,), (1,)), ((), ())), preferred_element_type=F32)


def dot_tn(a, b):
    return lax.dot_general(a, b, (((0,), (0,)), ((), ())), preferred_element_type=F32)


def tile(index, size):
    return pl.ds(pl.multiple_of(index * size, size), size)


def pick(index, values):
    out = 0
    for k, v in enumerate(values):
        out = out + jnp.where(index == k, v, 0)
    return out


def nearest(count):
    return [sorted((p for p in range(count) if p != i), key=lambda p: (abs(p - i), p)) for i in range(count)]


def make_kernel(n_sec, n_dp, n_mp):
    cores = 2 if n_mp % 2 == 0 else 1
    chips = n_mp // cores

    def kernel(
        text_in, image_in, scale_ref, hidden_in, w_in, w_out,
        image_out, input_out, first_out, second_out,
        text, image, hidden,
        text_low, cols, scores, sgrad, row_max, row_sum, row_lse, row_st, row_rx, col_st, col_rx,
        raw_in, raw_out, wi_all, wo_all, slope_own, slope_all, act_all, pre_all, grad_own,
        a_tx, a_rx, b_tx, b_rx, c_tx, c_rx, t_acc, g_all, g_new,
        w_acc, w_tx, w_rx, w_via, w_side, i_tx, i_rx,
        ld, gat_s, gat_r, cs_s, cs_r, rs_s, rs_r, wi_s, wi_a, wi_i,
        wo_s, yo_r, so_r, zo_r, fo_r, a_s, a_r, b_s, b_r, c_s, c_r, g_s, ga_r, gi_r, x_s, x_r,
        in_s, in_a, in_i, ix_s, ix_r, w_s, w_r, v_r, sd_s, sd_r, im_s, im_r, io_s, io_r,
    ):
        s = lax.axis_index("section")
        d = lax.axis_index("dp")
        m = lax.axis_index("mp")
        last = n_sec - 1
        rows, feats = text.shape
        own = image.shape[0]
        half = own // n_sec
        quarter = rows // n_mp
        piece = quarter // PIECES
        hid = slope_all.shape[1]
        share = feats // n_dp
        width = feats // n_sec
        mult = scale_ref[0]
        core = lax.rem(m, cores)
        chip = m // cores

        def copy(src, dst, send, recv, where):
            return pltpu.make_async_remote_copy(
                src_ref=src, dst_ref=dst, send_sem=send, recv_sem=recv,
                device_id=where, device_id_type=MESH,
            )

        def wait_all(ref, sem):
            pltpu.make_async_copy(ref, ref, sem).wait()

        def others(mine, count):
            return [lax.rem(mine + k, count) for k in range(1, count)]

        def sources(mine, count):
            return [lax.rem(mine + count - k, count) for k in range(1, count)]

        order = nearest(n_dp)
        near = [pick(d, [order[i][k] for i in range(n_dp)]) for k in range(n_dp - 1)]
        far = near[::-1]

        barrier = pltpu.get_barrier_semaphore()
        plane = [(t, p) for t in [s] + others(s, n_sec) for p in [m] + others(m, n_mp)][1:]
        for t, p in plane:
            pl.semaphore_signal(barrier, inc=1, device_id={"section": t, "mp": p}, device_id_type=MESH)
        for p in near:
            pl.semaphore_signal(barrier, inc=1, device_id={"dp": p}, device_id_type=MESH)
        via_hub = n_dp == 4
        by_side = via_hub and n_sec == 2
        mate = d + 1 - 2 * lax.rem(d, 2)
        if by_side:
            pl.semaphore_signal(barrier, inc=1, device_id={"section": 1 - s, "dp": mate}, device_id_type=MESH)

        loads = [
            pltpu.make_async_copy(image_in, image, ld.at[0]),
            pltpu.make_async_copy(w_in, raw_in, ld.at[1]),
            pltpu.make_async_copy(w_out, raw_out, ld.at[2]),
            pltpu.make_async_copy(text_in, text, ld.at[3]),
            pltpu.make_async_copy(hidden_in, hidden, ld.at[4]),
        ]
        for c in loads:
            c.start()

        mine_half = tile(s, half)
        loads[0].wait()
        own_unit, _ = unit_rows(image[mine_half, :])
        cols[tile(d, half), :] = own_unit.astype(BF16)
        pl.semaphore_wait(barrier, len(plane) + n_dp - 1 + (1 if by_side else 0))

        for p in far:
            copy(cols.at[tile(d, half), :], cols.at[tile(d, half), :], gat_s, gat_r.at[d], {"dp": p}).start()

        class Spread:
            def __init__(self, slot, send, across, inside):
                self.slot, self.send, self.across, self.inside = slot, send, across, inside

            def push(self, index, recv, to):
                copy(self.slot(index), self.slot(index), self.send, recv, {"mp": to}).start()

            def start(self):
                for k, q in enumerate(others(chip, chips)):
                    self.push(m, self.across.at[k], q * cores + core)
                for e in others(core, cores):
                    self.push(m, self.inside.at[chip], chip * cores + e)

            def relay(self):
                for k, q in enumerate(sources(chip, chips)):
                    index = q * cores + core
                    copy(self.slot(index), self.slot(index), self.send, self.across.at[k], {"mp": index}).wait_recv()
                    for e in others(core, cores):
                        self.push(index, self.inside.at[q], chip * cores + e)

            def finish(self):
                for e in sources(core, cores):
                    for q in range(chips):
                        slot = self.slot(q * cores + e)
                        copy(slot, slot, self.send, self.inside.at[q], {"mp": chip * cores + e}).wait_recv()

        pairs = 2 if n_dp % 2 == 0 else 1
        side = lax.rem(d, pairs)
        depth = feats // pairs

        def wo_part(index, k):
            return wo_all.at[index, tile(k, depth), :]

        loads[2].wait()
        wo_all[m] = raw_out[...].T
        def wo_push(ref, recv, to):
            copy(ref, ref, wo_s, recv, to).start()

        for k, q in enumerate(others(chip, chips)):
            wo_push(wo_part(m, side), yo_r.at[k], {"mp": q * cores + core})
        for e in others(core, cores):
            wo_push(wo_all.at[m], so_r, {"mp": chip * cores + e})

        loads[1].wait()
        wi_all[m] = raw_in[...].T

        def wi_spread_of(k):
            return Spread(lambda j: wi_all.at[j, pl.ds(k * (hid // 2), hid // 2), :], wi_s, wi_a.at[k], wi_i.at[k])

        wi_spread = [wi_spread_of(k) for k in range(2)]
        wi_spread[0].start()

        def wo_across():
            for k, q in enumerate(sources(chip, chips)):
                index = q * cores + core
                at = wo_part(index, side)
                copy(at, at, wo_s, yo_r.at[k], {"mp": index}).wait_recv()
                if pairs == 2:
                    wo_push(at, zo_r.at[k], {"dp": d + 1 - 2 * side})
                for e in others(core, cores):
                    wo_push(at, fo_r.at[k, 0], {"mp": chip * cores + e})

        def wo_along():
            for k, q in enumerate(sources(chip, chips)):
                at = wo_part(q * cores + core, 1 - side)
                if pairs == 2:
                    copy(at, at, wo_s, zo_r.at[k], {"dp": d + 1 - 2 * side}).wait_recv()
                    for e in others(core, cores):
                        wo_push(at, fo_r.at[k, 1], {"mp": chip * cores + e})

        def wo_finish():
            for e in sources(core, cores):
                to = {"mp": chip * cores + e}
                own_block = wo_all.at[chip * cores + e]
                copy(own_block, own_block, wo_s, so_r, to).wait_recv()
                for i, q in enumerate(sources(chip, chips)):
                    for k in range(pairs):
                        at = wo_part(q * cores + e, side if k == 0 else 1 - side)
                        copy(at, at, wo_s, fo_r.at[i, k], to).wait_recv()

        loads[3].wait()

        @pl.loop(0, n_mp)
        def _(r):
            unit, _ = unit_rows(text[tile(r, quarter), :])
            text_low[tile(r, quarter), :] = unit.astype(BF16)

        row_max[...] = jnp.full(row_max.shape, -1e30, F32)
        row_sum[...] = jnp.zeros(row_sum.shape, F32)

        def block_scores(p):
            block = cols[tile(p, half), :]
            peak = jnp.full((1, half), -1e30, F32)
            for r in range(n_mp):
                part = pl.ds(r * quarter, quarter)
                value = mult * dot_nt(text_low[part, :], block)
                scores[part, tile(p, half)] = value
                peak = jnp.maximum(peak, jnp.max(value, axis=0, keepdims=True))
            acc = jnp.zeros((1, half), F32)
            for r in range(n_mp):
                value = scores[pl.ds(r * quarter, quarter), tile(p, half)]
                acc = acc + jnp.sum(jnp.exp(value - peak), axis=0, keepdims=True)
            col_st[pl.ds(p, 1), :] = peak
            col_st[pl.ds(n_dp + p, 1), :] = acc

        def block_rows(p):
            for r in range(n_mp):
                part = pl.ds(r * quarter, quarter)
                old = row_max[part, :]
                best = old
                value = [scores[part, pl.ds(pl.multiple_of(p * half + k, LANES), LANES)] for k in range(0, half, LANES)]
                for v in value:
                    best = jnp.maximum(best, v)
                acc = row_sum[part, :] * jnp.exp(old - best)
                for v in value:
                    acc = acc + jnp.exp(v - best)
                row_max[part, :] = best
                row_sum[part, :] = acc

        block_scores(d)
        block_rows(d)

        def gelu_terms(pre):
            sigm = 1.0 / (1.0 + jnp.exp(-GELU * pre))
            return pre * sigm, sigm + GELU * pre * sigm * (1.0 - sigm)

        loads[4].wait()

        @pl.loop(0, n_mp)
        def _(r):
            act, slope = gelu_terms(dot_nn(hidden[tile(r, quarter), :], raw_in[...]))
            act_all[tile(r, quarter), :] = act.astype(BF16)
            slope_all[tile(r, quarter), :] = slope

        @pl.loop(0, n_dp - 1)
        def _(k):
            p = near[0]
            for i in range(1, n_dp - 1):
                p = jnp.where(k == i, near[i], p)
            copy(cols.at[tile(p, half), :], cols.at[tile(p, half), :], gat_s, gat_r.at[p], {"dp": p}).wait_recv()
            block_scores(p)

            @pl.when(k < n_dp - 2)
            def _():
                block_rows(p)

        col_rx[d] = col_st[...]
        for p in far:
            copy(col_st, col_rx.at[d], cs_s, cs_r, {"dp": p}).start()

        wo_across()
        block_rows(far[0])

        for r in range(n_mp):
            part = pl.ds(r * quarter, quarter)
            peak = jnp.max(row_max[part, :], axis=1, keepdims=True)
            acc = jnp.sum(row_sum[part, :] * jnp.exp(row_max[part, :] - peak), axis=1, keepdims=True)
            wide_peak = jnp.broadcast_to(peak, (quarter, LANES)).T
            wide_sum = jnp.broadcast_to(acc, (quarter, LANES)).T
            row_st[r : r + 1, :] = wide_peak[0:1, :]
            row_st[n_mp + r : n_mp + r + 1, :] = wide_sum[0:1, :]

        here = s * n_mp + m
        row_rx[here] = row_st[...]
        for k, (t, p) in enumerate(plane):
            copy(row_st, row_rx.at[here], rs_s, rs_r, {"section": t, "mp": p}).start()

        wi_spread[1].start()
        wi_spread[0].relay()

        def merge(rx, count, n):
            peak = rx[0, 0:n, :]
            for k in range(1, count):
                peak = jnp.maximum(peak, rx[k, 0:n, :])
            acc = jnp.zeros(peak.shape, F32)
            for k in range(count):
                acc = acc + rx[k, n : 2 * n, :] * jnp.exp(rx[k, 0:n, :] - peak)
            return peak + jnp.log(acc)

        wait_all(col_rx.at[pl.ds(0, n_dp - 1)], cs_r)
        col_lse = merge(col_rx, n_dp, n_dp)
        wait_all(row_rx.at[pl.ds(0, n_sec * n_mp - 1)], rs_r)
        merged = merge(row_rx, n_sec * n_mp, n_mp)
        for r in range(n_mp):
            row_lse[r] = jnp.broadcast_to(merged[r : r + 1, :], (LANES, quarter)).T

        def score_rows(r):
            line = row_lse[r]
            for p in range(n_dp):
                for k in range(0, half, LANES):
                    at = pl.ds(p * half + k, LANES)
                    value = scores[tile(r, quarter), at]
                    both = jnp.exp(value - line) + jnp.exp(value - col_lse[p : p + 1, k : k + LANES])
                    sgrad[tile(r, quarter), at] = (0.5 * both).astype(BF16)

        def score_diagonal():
            line = row_lse[m]
            text_id = lax.broadcasted_iota(jnp.int32, (quarter, LANES), 0)
            lse = col_lse[0:1, :]
            for p in range(1, n_dp):
                lse = jnp.where(d == p, col_lse[p : p + 1, :], lse)
            for k in range(0, half, LANES):
                at = pl.ds(pl.multiple_of(d * half + k, LANES), LANES)
                value = scores[tile(m, quarter), at]
                both = jnp.exp(value - line) + jnp.exp(value - lse[:, k : k + LANES])
                image_id = lax.broadcasted_iota(jnp.int32, (quarter, LANES), 1) + (s * half + k)
                out = 0.5 * both - jnp.where(text_id == image_id, 1.0, 0.0)
                sgrad[tile(m, quarter), at] = out.astype(BF16)

        def text_part(r):
            return dot_nn(sgrad[tile(r, quarter), :], cols[...])

        def rows_of(k):
            return tile(k, piece)

        def for_sibling(q):
            for e in others(core, cores):
                r = q * cores + e
                score_rows(r)
                a_tx[q] = text_part(r).astype(BF16)
                copy(a_tx.at[q], a_rx.at[q], a_s, a_r.at[q], {"mp": chip * cores + e}).start()

        def from_sibling(q):
            for e in others(core, cores):
                copy(a_tx.at[q], a_rx.at[q], a_s, a_r.at[q], {"mp": chip * cores + e}).wait_recv()
                t_acc[...] += a_rx[q].astype(F32)

        for i, q in enumerate(others(chip, chips)):
            for_sibling(q)
            score_rows(q * cores + core)
            t_acc[...] = text_part(q * cores + core)
            from_sibling(q)
            b_tx[q] = t_acc[...].astype(BF16)
            for k in range(PIECES):
                copy(b_tx.at[q, rows_of(k), :], b_rx.at[i, rows_of(k), :], b_s, b_r.at[i, k],
                     {"mp": q * cores + core}).start()
        for_sibling(chip)
        score_rows(m)
        score_diagonal()
        t_acc[...] = text_part(m)

        def image_part(p):
            return dot_tn(sgrad[:, tile(p, half)], text_low[...])

        for p in far:
            i_tx[p] = image_part(p).astype(BF16)
            copy(i_tx.at[p], i_rx.at[d], im_s, im_r, {"dp": p}).start()
        i_tx[d] = image_part(d).astype(BF16)

        from_sibling(chip)
        mine = tile(m, quarter)
        wi_spread[1].relay()
        wo_along()

        def gather_sum(k):
            total = t_acc[rows_of(k), :]
            for i, q in enumerate(sources(chip, chips)):
                copy(b_tx.at[q, rows_of(k), :], b_rx.at[i, rows_of(k), :], b_s, b_r.at[i, k],
                     {"mp": q * cores + core}).wait_recv()
                total = total + b_rx[i, rows_of(k), :].astype(F32)
            return total

        def to_last(k):
            return copy(c_tx.at[rows_of(k), :], c_rx.at[s, rows_of(k), :], c_s, c_r.at[s, k],
                        {"section": last})

        def to_below(k):
            return copy(g_new.at[rows_of(k), :], g_all.at[m, rows_of(k), :], x_s, x_r.at[k],
                        {"section": s - 1})

        @pl.when(s != last)
        def _():
            @pl.loop(0, PIECES)
            def _(k):
                c_tx[rows_of(k), :] = gather_sum(k).astype(BF16)
                to_last(k).start()

        def own_slope(j):
            _, slope = gelu_terms(dot_nt(hidden[mine, :], wi_all[j]))
            slope_own[j] = slope

        own_slope(m)
        for spread in wi_spread:
            spread.finish()

        @pl.loop(1, n_mp)
        def _(k):
            own_slope(lax.rem(m + k, n_mp))

        wo_finish()

        def g_push(k, index, recv, to):
            slot = g_all.at[index, rows_of(k), :]
            copy(slot, slot, g_s, recv, {"mp": to}).start()

        @pl.loop(0, PIECES // GROUP)
        def _(i):
            @pl.loop(i * GROUP, (i + 1) * GROUP)
            def _(k):
                at = tile(m * PIECES + k, piece)

                @pl.when(s == last)
                def _():
                    total = gather_sum(k)
                    for t in range(last):
                        copy(c_tx.at[rows_of(k), :], c_rx.at[t, rows_of(k), :], c_s, c_r.at[t, k],
                             {"section": t}).wait_recv()
                        total = total + c_rx[t, rows_of(k), :].astype(F32)
                    unit, length = unit_rows(text[at, :])
                    g_all[m, rows_of(k), :] = unit_backward(unit, length, mult * total).astype(BF16)

                @pl.when(s != last)
                def _():
                    copy(g_new.at[rows_of(k), :], g_all.at[m, rows_of(k), :], x_s, x_r.at[k],
                         {"section": s + 1}).wait_recv()

                for j, q in enumerate(others(chip, chips)):
                    g_push(k, m, ga_r.at[j, k], q * cores + core)

            group = tile(i, GROUP * piece)
            for e in others(core, cores):
                slot = g_all.at[m, group, :]
                copy(slot, slot, g_s, gi_r.at[chip, i], {"mp": chip * cores + e}).start()
            g = g_all[m, group, :]
            for j in range(n_mp):
                back = dot_nn(g, wo_all[j])
                grad_own[:, j * hid : (j + 1) * hid] = (back * slope_own[j, group, :]).astype(BF16)
            acc = dot_nn(grad_own[...], wi_all[...].reshape(n_mp * hid, feats))
            g_new[group, :] = (g.astype(F32) + acc).astype(BF16)

            @pl.when(s > 0)
            def _():
                for k in range(GROUP):
                    to_below(i * GROUP + k).start()

        groups = PIECES // GROUP

        def group_of(i):
            return pl.ds(i * GROUP * piece, GROUP * piece)

        def relay_group(i):
            for j, q in enumerate(sources(chip, chips)):
                index = q * cores + core
                for k in range(i * GROUP, (i + 1) * GROUP):
                    slot = g_all.at[index, rows_of(k), :]
                    copy(slot, slot, g_s, ga_r.at[j, k], {"mp": index}).wait_recv()
                slot = g_all.at[index, group_of(i), :]
                for e in others(core, cores):
                    copy(slot, slot, g_s, gi_r.at[q, i], {"mp": chip * cores + e}).start()

        def sibling_groups(q):
            for i in range(groups):
                for e in sources(core, cores):
                    slot = g_all.at[q * cores + e, group_of(i), :]
                    copy(slot, slot, g_s, gi_r.at[q, i], {"mp": chip * cores + e}).wait_recv()

        def chip_grad(q, at):
            left = g_all[pl.ds(q * cores, cores), :, at]
            return dot_tn(left.reshape(cores * quarter, left.shape[2]), act_all[tile(q, cores * quarter), :])

        for i in range(groups - 2):
            relay_group(i)
        sibling_groups(chip)
        relay_group(groups - 2)
        w_acc[...] = chip_grad(chip, pl.ds(0, feats))
        relay_group(groups - 1)

        def slab(k):
            return input_out.at[tile(k, quarter), :]

        def final(t):
            return copy(g_new.at[:, t * width : (t + 1) * width], slab(m), ix_s, ix_r,
                        {"section": t})

        @pl.when(s == 0)
        def _():
            for t in range(1, n_sec):
                final(t).start()
            input_out[mine, :] = g_new[:, 0:width]

        for q in sources(chip, chips):
            sibling_groups(q)

        low = d < n_dp // 2
        end = (d == 0) | (d == n_dp - 1)
        inner = jnp.logical_not(end)
        cross = [jnp.where(low, n_dp - 1, 0), jnp.where(low, n_dp - 2, 1)]

        def weight_grad(which, at):
            if which == 1:
                total = w_acc[at, :]
                for q in sources(chip, chips):
                    total = total + chip_grad(q, at)
                return total.astype(BF16)
            return dot_tn(hidden[:, at], pre_all[...]).astype(BF16)

        halves = [pl.ds(h * (share // 2), share // 2) for h in range(2)]

        def to_dp(which, p, slot):
            return copy(w_tx.at[p, which], w_rx.at[slot, which], w_s, w_r.at[which, slot], {"dp": p})

        def to_hub(which, k):
            return [
                copy(w_tx.at[cross[k], which, at, :], w_via.at[which, k, at, :], w_s, v_r.at[which, k, h], {"dp": mate})
                for h, at in enumerate(halves)
            ]

        def to_cross(which, k, h):
            return copy(w_tx.at[cross[k], which, halves[h], :], w_rx.at[1, which, halves[h], :], w_s,
                        w_r.at[which, 1 + h], {"dp": cross[k]})

        def to_side():
            return copy(w_tx.at[mate, 1], w_side, w_s, sd_r, {"section": 1})

        def from_side():
            return copy(w_side, w_rx.at[0, 1], sd_s, w_r.at[1, 0], {"section": 0, "dp": mate})

        def last_weights():
            if by_side:
                pl.when(end & (s == 0))(lambda: to_dp(0, mate, 0).start())
                pl.when(end & (s == 1))(lambda: to_dp(1, mate, 0).start())
            elif via_hub:

                @pl.when(end)
                def _():
                    to_dp(1, mate, 0).start()
                    to_dp(0, mate, 0).start()

        def side_weights():
            if by_side:

                @pl.when(end & (s == 1))
                def _():
                    to_side().wait_recv()
                    from_side().start()
                    to_dp(0, mate, 0).start()

        def send_weights(which):
            if via_hub:
                for k in range(2):
                    w_tx[cross[k], which] = weight_grad(which, tile(cross[k], share))

                    @pl.when(end)
                    def _():
                        for c in to_hub(which, 0) if k == 0 else to_hub(1, 1) + to_hub(0, 1) if which == 0 else []:
                            c.start()

                w_tx[mate, which] = weight_grad(which, tile(mate, share))

                @pl.when(inner)
                def _():
                    to_dp(which, mate, 0).start()

                if by_side and which == 1:

                    @pl.when(end & (s == 0))
                    def _():
                        to_side().start()

                w_tx[d, which] = weight_grad(which, tile(d, share))
            else:
                grad = weight_grad(which, pl.ds(0, feats))
                for p in range(n_dp):
                    w_tx[p, which] = grad[p * share : (p + 1) * share, :]
                for p in far:
                    to_dp(which, p, d).start()

        def pass_on(which, k, h):
            if via_hub:

                @pl.when(inner)
                def _():
                    to_hub(which, k)[h].wait_recv()
                    both = w_tx[cross[k], which, halves[h], :].astype(F32) + w_via[which, k, halves[h], :].astype(F32)
                    w_tx[cross[k], which, halves[h], :] = both.astype(BF16)
                    to_cross(which, k, h).start()

        send_weights(1)

        @pl.loop(0, n_mp)
        def _(r):
            back = dot_nn(g_all[r], wo_all[m])
            pre_all[tile(r, quarter), :] = (back * slope_all[tile(r, quarter), :]).astype(BF16)

        pass_on(1, 0, 0)
        send_weights(0)
        last_weights()
        pass_on(1, 0, 1)
        for h in range(2):
            pass_on(0, 0, h)
        in_spread = Spread(slab, in_s, in_a, in_i)

        @pl.when(s != 0)
        def _():
            copy(g_new.at[:, 0:width], slab(m), ix_s, ix_r, {"section": 0}).wait_recv()

        in_spread.start()

        total = i_tx[d].astype(F32)
        wait_all(i_rx.at[pl.ds(0, n_dp - 1)], im_r)
        for p in near:
            total = total + i_rx[p].astype(F32)
        unit, length = unit_rows(image[mine_half, :])
        image_out[mine_half, :] = unit_backward(unit, length, mult * total).astype(BF16)
        for t in others(s, n_sec):
            copy(image_out.at[mine_half, :], image_out.at[mine_half, :], io_s, io_r, {"section": t}).start()

        side_weights()
        for which in (1, 0):
            for h in range(2):
                pass_on(which, 1, h)
        in_spread.relay()
        in_spread.finish()

        wait_all(image_out.at[pl.ds(0, (n_sec - 1) * half), :], io_r)

        wait_all(cols.at[pl.ds(0, (n_dp - 1) * half), :], gat_s)
        wait_all(col_rx.at[pl.ds(0, n_dp - 1)], cs_s)
        wait_all(row_rx.at[pl.ds(0, n_sec * n_mp - 1)], rs_s)
        wait_all(wi_all.at[pl.ds(0, n_mp - 1)], wi_s)
        wait_all(wo_all.at[pl.ds(0, n_mp - 1)], wo_s)
        if cores > 1:
            wait_all(a_tx, a_s)
        if chips > 1:
            wait_all(b_tx.at[pl.ds(0, chips - 1)], b_s)
        wait_all(g_all.at[pl.ds(0, n_mp - 1)], g_s)
        wait_all(i_tx.at[pl.ds(0, n_dp - 1)], im_s)
        wait_all(input_out.at[pl.ds(0, (n_mp - 1) * quarter), :], in_s)
        wait_all(image_out.at[pl.ds(0, (n_sec - 1) * half), :], io_s)

        @pl.when(s != last)
        def _():
            wait_all(c_tx, c_s)

        @pl.when(s > 0)
        def _():
            wait_all(g_new, x_s)

        @pl.when(s == 0)
        def _():
            wait_all(g_new.at[:, pl.ds(0, (n_sec - 1) * width)], ix_s)

        for which, out in ((1, second_out), (0, first_out)):
            out[...] = w_tx[d, which].astype(F32)

            for p in [0] if via_hub else near:
                copy(w_rx.at[p, which], w_rx.at[p, which], w_s, w_r.at[which, p], {"dp": mate}).wait_recv()
                out[...] += w_rx[p, which].astype(F32)
            for h, at in enumerate(halves if via_hub else []):
                to_cross(which, 0, h).wait_recv()
                out[at, :] += w_rx[1, which, at, :].astype(F32)
        wait_all(w_tx.at[pl.ds(0, n_dp - 1)], w_s)
        if by_side:
            pl.when(end & (s == 1))(lambda: wait_all(w_side, sd_s))

    return kernel


def store(image, inputs, first, second, image_out, input_out, first_out, second_out, sems):
    copies = [
        pltpu.make_async_copy(image, image_out, sems.at[0]),
        pltpu.make_async_copy(inputs, input_out, sems.at[1]),
        pltpu.make_async_copy(first, first_out.at[0], sems.at[2]),
        pltpu.make_async_copy(second, second_out.at[0], sems.at[3]),
    ]
    for c in copies:
        c.start()
    for c in copies:
        c.wait()


def solution(mesh):
    n_sec, n_dp, n_mp = mesh.shape["section"], mesh.shape["dp"], mesh.shape["mp"]

    def body(text, image, scale, hidden, w_in, w_out):
        rows, feats = text.shape
        own = image.shape[0]
        hid = w_in.shape[2]
        quarter, half, share = rows // n_mp, own // n_sec, feats // n_dp
        columns = half * n_dp
        cores = 2 if n_mp % 2 == 0 else 1
        chips = n_mp // cores
        away = max(chips - 1, 1)
        dma = pltpu.SemaphoreType.DMA
        vmem = pl.BlockSpec(memory_space=pltpu.VMEM)
        hbm = pl.BlockSpec(memory_space=pltpu.HBM)
        out = pl.pallas_call(
            make_kernel(n_sec, n_dp, n_mp),
            out_shape=(
                pltpu.VMEM((own, feats), BF16),
                pltpu.VMEM((rows, feats // n_sec), BF16),
                pltpu.VMEM((share, hid), F32),
                pltpu.VMEM((share, hid), F32),
            ),
            in_specs=[hbm, hbm, pl.BlockSpec(memory_space=pltpu.SMEM), hbm, hbm, hbm],
            out_specs=(vmem,) * 4,
            scratch_shapes=[
                pltpu.VMEM((rows, feats), BF16),
                pltpu.VMEM((own, feats), BF16),
                pltpu.VMEM((rows, feats), BF16),
                pltpu.VMEM((rows, feats), BF16),
                pltpu.VMEM((columns, feats), BF16),
                pltpu.VMEM((rows, columns), F32),
                pltpu.VMEM((rows, columns), BF16),
                pltpu.VMEM((rows, LANES), F32),
                pltpu.VMEM((rows, LANES), F32),
                pltpu.VMEM((n_mp, quarter, LANES), F32),
                pltpu.VMEM((2 * n_mp, quarter), F32),
                pltpu.VMEM((n_sec * n_mp, 2 * n_mp, quarter), F32),
                pltpu.VMEM((2 * n_dp, half), F32),
                pltpu.VMEM((n_dp, 2 * n_dp, half), F32),
                pltpu.VMEM((feats, hid), BF16),
                pltpu.VMEM((hid, feats), BF16),
                pltpu.VMEM((n_mp, hid, feats), BF16),
                pltpu.VMEM((n_mp, feats, hid), BF16),
                pltpu.VMEM((n_mp, quarter, hid), F32),
                pltpu.VMEM((rows, hid), F32),
                pltpu.VMEM((rows, hid), BF16),
                pltpu.VMEM((rows, hid), BF16),
                pltpu.VMEM((quarter // PIECES * GROUP, n_mp * hid), BF16),
                pltpu.VMEM((chips, quarter, feats), BF16),
                pltpu.VMEM((chips, quarter, feats), BF16),
                pltpu.VMEM((chips, quarter, feats), BF16),
                pltpu.VMEM((chips, quarter, feats), BF16),
                pltpu.VMEM((quarter, feats), BF16),
                pltpu.VMEM((n_sec, quarter, feats), BF16),
                pltpu.VMEM((quarter, feats), F32),
                pltpu.VMEM((n_mp, quarter, feats), BF16),
                pltpu.VMEM((quarter, feats), BF16),
                pltpu.VMEM((feats, hid), F32),
                pltpu.VMEM((n_dp, 2, share, hid), BF16),
                pltpu.VMEM((n_dp, 2, share, hid), BF16),
                pltpu.VMEM((2, 2, share, hid), BF16),
                pltpu.VMEM((share, hid), BF16),
                pltpu.VMEM((n_dp, half, feats), BF16),
                pltpu.VMEM((n_dp, half, feats), BF16),
                dma((5,)),
                dma, dma((n_dp,)),
                dma, dma,
                dma, dma,
                dma, dma((2, away)), dma((2, chips)),
                dma, dma((away,)), dma, dma((away,)), dma((away, 2)),
                dma, dma((chips,)),
                dma, dma((away, PIECES)),
                dma, dma((n_sec - 1, PIECES)),
                dma, dma((away, PIECES)), dma((chips, PIECES // GROUP)),
                dma, dma((PIECES,)),
                dma, dma((away,)), dma((chips,)),
                dma, dma,
                dma, dma((2, 3 if n_dp == 4 else n_dp)), dma((2, 2, 2)), dma, dma,
                dma, dma,
                dma, dma,
            ],
            compiler_params=pltpu.CompilerParams(
                collective_id=0, has_side_effects=True, vmem_limit_bytes=50000000
            ),
        )(*(pltpu.with_memory_space_constraint(x, pltpu.HBM) for x in (text, image)), scale,
          *(pltpu.with_memory_space_constraint(x[0], pltpu.HBM) for x in (hidden, w_in, w_out)))
        return tuple(
            pl.pallas_call(
                store,
                out_shape=(
                    jax.ShapeDtypeStruct((own, feats), BF16),
                    jax.ShapeDtypeStruct((rows, feats // n_sec), BF16),
                    jax.ShapeDtypeStruct((1, share, hid), F32),
                    jax.ShapeDtypeStruct((1, share, hid), F32),
                ),
                in_specs=[vmem] * 4,
                out_specs=(hbm,) * 4,
                scratch_shapes=[dma((4,))],
                compiler_params=pltpu.CompilerParams(has_side_effects=True),
            )(*(pltpu.with_memory_space_constraint(x, pltpu.VMEM) for x in out))
        )

    return jax.shard_map(
        body,
        mesh=mesh,
        in_specs=(
            P("dp", None),
            P(("dp", "mp"), None),
            P(),
            P("section", "dp", None),
            P("section", None, "mp"),
            P("section", "mp", None),
        ),
        out_specs=(
            P(("dp", "mp"), None),
            P("dp", "section"),
            P("section", "dp", "mp"),
            P("section", "dp", "mp"),
        ),
        check_vma=False,
    )
```

```python
import jax
import jax.numpy as jnp
from jax import lax
from jax.experimental import pallas as pl
from jax.experimental.pallas import tpu as pltpu
from jax.sharding import PartitionSpec as P

MESH = pl.DeviceIdType.MESH
F32 = jnp.float32
BF16 = jnp.bfloat16
GELU = 1.702
LANES = 128
PIECES = 8
GROUP = 2


def unit_rows(values):
    wide = values.astype(F32)
    length = jnp.sqrt(jnp.sum(wide * wide, axis=1, keepdims=True) + 1.0)
    return (wide / length, length)


def unit_backward(unit, length, grad_unit):
    return (grad_unit - unit * jnp.sum(unit * grad_unit, axis=1, keepdims=True)) / length


def dot_nn(a, b):
    return lax.dot_general(a, b, (((1,), (0,)), ((), ())), preferred_element_type=F32)


def dot_nt(a, b):
    return lax.dot_general(a, b, (((1,), (1,)), ((), ())), preferred_element_type=F32)


def dot_tn(a, b):
    return lax.dot_general(a, b, (((0,), (0,)), ((), ())), preferred_element_type=F32)


def tile(index, size):
    return pl.ds(pl.multiple_of(index * size, size), size)


def pick(index, values):
    out = 0
    for k, v in enumerate(values):
        out = out + jnp.where(index == k, v, 0)
    return out


def nearest(count):
    return [sorted((p for p in range(count) if p != i), key=lambda p: (abs(p - i), p)) for i in range(count)]


def make_kernel(n_sec, n_dp, n_mp):
    cores = 2 if n_mp % 2 == 0 else 1
    chips = n_mp // cores

    def kernel(
        text_in, image_in, scale_ref, hidden_in, w_in, w_out,
        image_out, input_out, first_out, second_out,
        text, image, hidden,
        text_low, cols, scores, sgrad, row_max, row_sum, row_lse, row_st, row_rx, col_st, col_rx,
        raw_in, raw_out, wi_all, wo_all, slope_own, slope_all, act_all, pre_all, grad_own,
        a_tx, a_rx, b_tx, b_rx, c_tx, c_rx, t_acc, g_all, g_new,
        w_acc, w_tx, w_rx, w_via, w_side, i_tx, i_rx,
        ld, gat_s, gat_r, cs_s, cs_r, rs_s, rs_r, wi_s, wi_a, wi_i,
        wo_s, yo_r, so_r, zo_r, fo_r, a_s, a_r, b_s, b_r, c_s, c_r, g_s, ga_r, gi_r, x_s, x_r,
        in_s, in_a, in_i, ix_s, ix_r, w_s, w_r, v_r, sd_s, sd_r, im_s, im_r, io_s, io_r,
    ):
        s = lax.axis_index("section")
        d = lax.axis_index("dp")
        m = lax.axis_index("mp")
        last = n_sec - 1
        rows, feats = text.shape
        own = image.shape[0]
        half = own // n_sec
        quarter = rows // n_mp
        piece = quarter // PIECES
        hid = slope_all.shape[1]
        share = feats // n_dp
        width = feats // n_sec
        mult = scale_ref[0]
        core = lax.rem(m, cores)
        chip = m // cores

        def copy(src, dst, send, recv, where):
            return pltpu.make_async_remote_copy(
                src_ref=src, dst_ref=dst, send_sem=send, recv_sem=recv,
                device_id=where, device_id_type=MESH,
            )

        def wait_all(ref, sem):
            pltpu.make_async_copy(ref, ref, sem).wait()

        def others(mine, count):
            return [lax.rem(mine + k, count) for k in range(1, count)]

        def sources(mine, count):
            return [lax.rem(mine + count - k, count) for k in range(1, count)]

        order = nearest(n_dp)
        near = [pick(d, [order[i][k] for i in range(n_dp)]) for k in range(n_dp - 1)]
        far = near[::-1]

        barrier = pltpu.get_barrier_semaphore()
        plane = [(t, p) for t in [s] + others(s, n_sec) for p in [m] + others(m, n_mp)][1:]
        for t, p in plane:
            pl.semaphore_signal(barrier, inc=1, device_id={"section": t, "mp": p}, device_id_type=MESH)
        for p in near:
            pl.semaphore_signal(barrier, inc=1, device_id={"dp": p}, device_id_type=MESH)
        via_hub = n_dp == 4
        by_side = via_hub and n_sec == 2
        mate = d + 1 - 2 * lax.rem(d, 2)
        if by_side:
            pl.semaphore_signal(barrier, inc=1, device_id={"section": 1 - s, "dp": mate}, device_id_type=MESH)

        loads = [
            pltpu.make_async_copy(image_in, image, ld.at[0]),
            pltpu.make_async_copy(w_in, raw_in, ld.at[1]),
            pltpu.make_async_copy(w_out, raw_out, ld.at[2]),
            pltpu.make_async_copy(text_in, text, ld.at[3]),
            pltpu.make_async_copy(hidden_in, hidden, ld.at[4]),
        ]
        for c in loads:
            c.start()

        mine_half = tile(s, half)
        loads[0].wait()
        own_unit, _ = unit_rows(image[mine_half, :])
        cols[tile(d, half), :] = own_unit.astype(BF16)
        pl.semaphore_wait(barrier, len(plane) + n_dp - 1 + (1 if by_side else 0))

        for p in far:
            copy(cols.at[tile(d, half), :], cols.at[tile(d, half), :], gat_s, gat_r.at[d], {"dp": p}).start()

        class Spread:
            def __init__(self, slot, send, across, inside):
                self.slot, self.send, self.across, self.inside = slot, send, across, inside

            def push(self, index, recv, to):
                copy(self.slot(index), self.slot(index), self.send, recv, {"mp": to}).start()

            def start(self):
                for k, q in enumerate(others(chip, chips)):
                    self.push(m, self.across.at[k], q * cores + core)
                for e in others(core, cores):
                    self.push(m, self.inside.at[chip], chip * cores + e)

            def relay(self):
                for k, q in enumerate(sources(chip, chips)):
                    index = q * cores + core
                    copy(self.slot(index), self.slot(index), self.send, self.across.at[k], {"mp": index}).wait_recv()
                    for e in others(core, cores):
                        self.push(index, self.inside.at[q], chip * cores + e)

            def finish(self):
                for e in sources(core, cores):
                    for q in range(chips):
                        slot = self.slot(q * cores + e)
                        copy(slot, slot, self.send, self.inside.at[q], {"mp": chip * cores + e}).wait_recv()

        pairs = 2 if n_dp % 2 == 0 else 1
        side = lax.rem(d, pairs)
        depth = feats // pairs

        def wo_part(index, k):
            return wo_all.at[index, tile(k, depth), :]

        loads[2].wait()
        wo_all[m] = raw_out[...].T
        def wo_push(ref, recv, to):
            copy(ref, ref, wo_s, recv, to).start()

        for k, q in enumerate(others(chip, chips)):
            wo_push(wo_part(m, side), yo_r.at[k], {"mp": q * cores + core})
        for e in others(core, cores):
            wo_push(wo_all.at[m], so_r, {"mp": chip * cores + e})

        loads[1].wait()
        wi_all[m] = raw_in[...].T

        def wi_spread_of(k):
            return Spread(lambda j: wi_all.at[j, pl.ds(k * (hid // 2), hid // 2), :], wi_s, wi_a.at[k], wi_i.at[k])

        wi_spread = [wi_spread_of(k) for k in range(2)]
        wi_spread[0].start()

        def wo_across():
            for k, q in enumerate(sources(chip, chips)):
                index = q * cores + core
                at = wo_part(index, side)
                copy(at, at, wo_s, yo_r.at[k], {"mp": index}).wait_recv()
                if pairs == 2:
                    wo_push(at, zo_r.at[k], {"dp": d + 1 - 2 * side})
                for e in others(core, cores):
                    wo_push(at, fo_r.at[k, 0], {"mp": chip * cores + e})

        def wo_along():
            for k, q in enumerate(sources(chip, chips)):
                at = wo_part(q * cores + core, 1 - side)
                if pairs == 2:
                    copy(at, at, wo_s, zo_r.at[k], {"dp": d + 1 - 2 * side}).wait_recv()
                    for e in others(core, cores):
                        wo_push(at, fo_r.at[k, 1], {"mp": chip * cores + e})

        def wo_finish():
            for e in sources(core, cores):
                to = {"mp": chip * cores + e}
                own_block = wo_all.at[chip * cores + e]
                copy(own_block, own_block, wo_s, so_r, to).wait_recv()
                for i, q in enumerate(sources(chip, chips)):
                    for k in range(pairs):
                        at = wo_part(q * cores + e, side if k == 0 else 1 - side)
                        copy(at, at, wo_s, fo_r.at[i, k], to).wait_recv()

        loads[3].wait()

        @pl.loop(0, n_mp)
        def _(r):
            unit, _ = unit_rows(text[tile(r, quarter), :])
            text_low[tile(r, quarter), :] = unit.astype(BF16)

        row_max[...] = jnp.full(row_max.shape, -1e30, F32)
        row_sum[...] = jnp.zeros(row_sum.shape, F32)

        def block_scores(p):
            block = cols[tile(p, half), :]
            peak = jnp.full((1, half), -1e30, F32)
            for r in range(n_mp):
                part = pl.ds(r * quarter, quarter)
                value = mult * dot_nt(text_low[part, :], block)
                scores[part, tile(p, half)] = value
                peak = jnp.maximum(peak, jnp.max(value, axis=0, keepdims=True))
            acc = jnp.zeros((1, half), F32)
            for r in range(n_mp):
                value = scores[pl.ds(r * quarter, quarter), tile(p, half)]
                acc = acc + jnp.sum(jnp.exp(value - peak), axis=0, keepdims=True)
            col_st[pl.ds(p, 1), :] = peak
            col_st[pl.ds(n_dp + p, 1), :] = acc

        def block_rows(p):
            for r in range(n_mp):
                part = pl.ds(r * quarter, quarter)
                old = row_max[part, :]
                best = old
                value = [scores[part, pl.ds(pl.multiple_of(p * half + k, LANES), LANES)] for k in range(0, half, LANES)]
                for v in value:
                    best = jnp.maximum(best, v)
                acc = row_sum[part, :] * jnp.exp(old - best)
                for v in value:
                    acc = acc + jnp.exp(v - best)
                row_max[part, :] = best
                row_sum[part, :] = acc

        block_scores(d)
        block_rows(d)

        def gelu_terms(pre):
            sigm = 1.0 / (1.0 + jnp.exp(-GELU * pre))
            return pre * sigm, sigm + GELU * pre * sigm * (1.0 - sigm)

        loads[4].wait()

        @pl.loop(0, n_mp)
        def _(r):
            act, slope = gelu_terms(dot_nn(hidden[tile(r, quarter), :], raw_in[...]))
            act_all[tile(r, quarter), :] = act.astype(BF16)
            slope_all[tile(r, quarter), :] = slope

        @pl.loop(0, n_dp - 1)
        def _(k):
            p = near[0]
            for i in range(1, n_dp - 1):
                p = jnp.where(k == i, near[i], p)
            copy(cols.at[tile(p, half), :], cols.at[tile(p, half), :], gat_s, gat_r.at[p], {"dp": p}).wait_recv()
            block_scores(p)

            @pl.when(k < n_dp - 2)
            def _():
                block_rows(p)

        col_rx[d] = col_st[...]
        for p in far:
            copy(col_st, col_rx.at[d], cs_s, cs_r, {"dp": p}).start()

        wo_across()
        block_rows(far[0])

        for r in range(n_mp):
            part = pl.ds(r * quarter, quarter)
            peak = jnp.max(row_max[part, :], axis=1, keepdims=True)
            acc = jnp.sum(row_sum[part, :] * jnp.exp(row_max[part, :] - peak), axis=1, keepdims=True)
            wide_peak = jnp.broadcast_to(peak, (quarter, LANES)).T
            wide_sum = jnp.broadcast_to(acc, (quarter, LANES)).T
            row_st[r : r + 1, :] = wide_peak[0:1, :]
            row_st[n_mp + r : n_mp + r + 1, :] = wide_sum[0:1, :]

        here = s * n_mp + m
        row_rx[here] = row_st[...]
        for k, (t, p) in enumerate(plane):
            copy(row_st, row_rx.at[here], rs_s, rs_r, {"section": t, "mp": p}).start()

        wi_spread[1].start()
        wi_spread[0].relay()

        def merge(rx, count, n):
            peak = rx[0, 0:n, :]
            for k in range(1, count):
                peak = jnp.maximum(peak, rx[k, 0:n, :])
            acc = jnp.zeros(peak.shape, F32)
            for k in range(count):
                acc = acc + rx[k, n : 2 * n, :] * jnp.exp(rx[k, 0:n, :] - peak)
            return peak + jnp.log(acc)

        wait_all(row_rx.at[pl.ds(0, n_sec * n_mp - 1)], rs_r)
        merged = merge(row_rx, n_sec * n_mp, n_mp)
        for r in range(n_mp):
            row_lse[r] = jnp.broadcast_to(merged[r : r + 1, :], (LANES, quarter)).T

        wait_all(col_rx.at[pl.ds(0, n_dp - 1)], cs_r)
        col_lse = merge(col_rx, n_dp, n_dp)

        def score_rows(r):
            line = row_lse[r]
            for p in range(n_dp):
                for k in range(0, half, LANES):
                    at = pl.ds(p * half + k, LANES)
                    value = scores[tile(r, quarter), at]
                    both = jnp.exp(value - line) + jnp.exp(value - col_lse[p : p + 1, k : k + LANES])
                    sgrad[tile(r, quarter), at] = (0.5 * both).astype(BF16)

        def score_diagonal():
            line = row_lse[m]
            text_id = lax.broadcasted_iota(jnp.int32, (quarter, LANES), 0)
            lse = col_lse[0:1, :]
            for p in range(1, n_dp):
                lse = jnp.where(d == p, col_lse[p : p + 1, :], lse)
            for k in range(0, half, LANES):
                at = pl.ds(pl.multiple_of(d * half + k, LANES), LANES)
                value = scores[tile(m, quarter), at]
                both = jnp.exp(value - line) + jnp.exp(value - lse[:, k : k + LANES])
                image_id = lax.broadcasted_iota(jnp.int32, (quarter, LANES), 1) + (s * half + k)
                out = 0.5 * both - jnp.where(text_id == image_id, 1.0, 0.0)
                sgrad[tile(m, quarter), at] = out.astype(BF16)

        def text_part(r):
            return dot_nn(sgrad[tile(r, quarter), :], cols[...])

        def rows_of(k):
            return tile(k, piece)

        def for_sibling(q):
            for e in others(core, cores):
                r = q * cores + e
                score_rows(r)
                a_tx[q] = text_part(r).astype(BF16)
                copy(a_tx.at[q], a_rx.at[q], a_s, a_r.at[q], {"mp": chip * cores + e}).start()

        def from_sibling(q):
            for e in others(core, cores):
                copy(a_tx.at[q], a_rx.at[q], a_s, a_r.at[q], {"mp": chip * cores + e}).wait_recv()
                t_acc[...] += a_rx[q].astype(F32)

        for i, q in enumerate(others(chip, chips)):
            for_sibling(q)
            score_rows(q * cores + core)
            t_acc[...] = text_part(q * cores + core)
            from_sibling(q)
            b_tx[q] = t_acc[...].astype(BF16)
            for k in range(PIECES):
                copy(b_tx.at[q, rows_of(k), :], b_rx.at[i, rows_of(k), :], b_s, b_r.at[i, k],
                     {"mp": q * cores + core}).start()
        for_sibling(chip)
        score_rows(m)
        score_diagonal()
        t_acc[...] = text_part(m)

        def image_part(p):
            return dot_tn(sgrad[:, tile(p, half)], text_low[...])

        for p in far:
            i_tx[p] = image_part(p).astype(BF16)
            copy(i_tx.at[p], i_rx.at[d], im_s, im_r, {"dp": p}).start()
        i_tx[d] = image_part(d).astype(BF16)

        from_sibling(chip)
        mine = tile(m, quarter)
        wi_spread[1].relay()
        wo_along()

        def gather_sum(k):
            total = t_acc[rows_of(k), :]
            for i, q in enumerate(sources(chip, chips)):
                copy(b_tx.at[q, rows_of(k), :], b_rx.at[i, rows_of(k), :], b_s, b_r.at[i, k],
                     {"mp": q * cores + core}).wait_recv()
                total = total + b_rx[i, rows_of(k), :].astype(F32)
            return total

        def to_last(k):
            return copy(c_tx.at[rows_of(k), :], c_rx.at[s, rows_of(k), :], c_s, c_r.at[s, k],
                        {"section": last})

        def to_below(k):
            return copy(g_new.at[rows_of(k), :], g_all.at[m, rows_of(k), :], x_s, x_r.at[k],
                        {"section": s - 1})

        @pl.when(s != last)
        def _():
            @pl.loop(0, PIECES)
            def _(k):
                c_tx[rows_of(k), :] = gather_sum(k).astype(BF16)
                to_last(k).start()

        def own_slope(j):
            _, slope = gelu_terms(dot_nt(hidden[mine, :], wi_all[j]))
            slope_own[j] = slope

        own_slope(m)
        for spread in wi_spread:
            spread.finish()

        @pl.loop(1, n_mp)
        def _(k):
            own_slope(lax.rem(m + k, n_mp))

        wo_finish()

        def g_push(k, index, recv, to):
            slot = g_all.at[index, rows_of(k), :]
            copy(slot, slot, g_s, recv, {"mp": to}).start()

        @pl.loop(0, PIECES // GROUP)
        def _(i):
            @pl.loop(i * GROUP, (i + 1) * GROUP)
            def _(k):
                at = tile(m * PIECES + k, piece)

                @pl.when(s == last)
                def _():
                    total = gather_sum(k)
                    for t in range(last):
                        copy(c_tx.at[rows_of(k), :], c_rx.at[t, rows_of(k), :], c_s, c_r.at[t, k],
                             {"section": t}).wait_recv()
                        total = total + c_rx[t, rows_of(k), :].astype(F32)
                    unit, length = unit_rows(text[at, :])
                    g_all[m, rows_of(k), :] = unit_backward(unit, length, mult * total).astype(BF16)

                @pl.when(s != last)
                def _():
                    copy(g_new.at[rows_of(k), :], g_all.at[m, rows_of(k), :], x_s, x_r.at[k],
                         {"section": s + 1}).wait_recv()

                for j, q in enumerate(others(chip, chips)):
                    g_push(k, m, ga_r.at[j, k], q * cores + core)

            group = tile(i, GROUP * piece)
            for e in others(core, cores):
                slot = g_all.at[m, group, :]
                copy(slot, slot, g_s, gi_r.at[chip, i], {"mp": chip * cores + e}).start()
            g = g_all[m, group, :]
            for j in range(n_mp):
                back = dot_nn(g, wo_all[j])
                grad_own[:, j * hid : (j + 1) * hid] = (back * slope_own[j, group, :]).astype(BF16)
            acc = dot_nn(grad_own[...], wi_all[...].reshape(n_mp * hid, feats))
            g_new[group, :] = (g.astype(F32) + acc).astype(BF16)

            @pl.when(s > 0)
            def _():
                for k in range(GROUP):
                    to_below(i * GROUP + k).start()

        groups = PIECES // GROUP

        def group_of(i):
            return pl.ds(i * GROUP * piece, GROUP * piece)

        def relay_group(i):
            for j, q in enumerate(sources(chip, chips)):
                index = q * cores + core
                for k in range(i * GROUP, (i + 1) * GROUP):
                    slot = g_all.at[index, rows_of(k), :]
                    copy(slot, slot, g_s, ga_r.at[j, k], {"mp": index}).wait_recv()
                slot = g_all.at[index, group_of(i), :]
                for e in others(core, cores):
                    copy(slot, slot, g_s, gi_r.at[q, i], {"mp": chip * cores + e}).start()

        def sibling_groups(q):
            for i in range(groups):
                for e in sources(core, cores):
                    slot = g_all.at[q * cores + e, group_of(i), :]
                    copy(slot, slot, g_s, gi_r.at[q, i], {"mp": chip * cores + e}).wait_recv()

        def chip_grad(q, at):
            left = g_all[pl.ds(q * cores, cores), :, at]
            return dot_tn(left.reshape(cores * quarter, left.shape[2]), act_all[tile(q, cores * quarter), :])

        for i in range(groups - 2):
            relay_group(i)
        sibling_groups(chip)
        relay_group(groups - 2)
        w_acc[...] = chip_grad(chip, pl.ds(0, feats))
        relay_group(groups - 1)

        def slab(k):
            return input_out.at[tile(k, quarter), :]

        def final(t):
            return copy(g_new.at[:, t * width : (t + 1) * width], slab(m), ix_s, ix_r,
                        {"section": t})

        @pl.when(s == 0)
        def _():
            for t in range(1, n_sec):
                final(t).start()
            input_out[mine, :] = g_new[:, 0:width]

        for q in sources(chip, chips):
            sibling_groups(q)

        low = d < n_dp // 2
        end = (d == 0) | (d == n_dp - 1)
        inner = jnp.logical_not(end)
        cross = [jnp.where(low, n_dp - 1, 0), jnp.where(low, n_dp - 2, 1)]

        def weight_grad(which, at):
            if which == 1:
                total = w_acc[at, :]
                for q in sources(chip, chips):
                    total = total + chip_grad(q, at)
                return total.astype(BF16)
            return dot_tn(hidden[:, at], pre_all[...]).astype(BF16)

        halves = [pl.ds(h * (share // 2), share // 2) for h in range(2)]

        def to_dp(which, p, slot):
            return copy(w_tx.at[p, which], w_rx.at[slot, which], w_s, w_r.at[which, slot], {"dp": p})

        def to_hub(which, k):
            return [
                copy(w_tx.at[cross[k], which, at, :], w_via.at[which, k, at, :], w_s, v_r.at[which, k, h], {"dp": mate})
                for h, at in enumerate(halves)
            ]

        def to_cross(which, k, h):
            return copy(w_tx.at[cross[k], which, halves[h], :], w_rx.at[1, which, halves[h], :], w_s,
                        w_r.at[which, 1 + h], {"dp": cross[k]})

        def to_side():
            return copy(w_tx.at[mate, 1], w_side, w_s, sd_r, {"section": 1})

        def from_side():
            return copy(w_side, w_rx.at[0, 1], sd_s, w_r.at[1, 0], {"section": 0, "dp": mate})

        def last_weights():
            if by_side:
                pl.when(end & (s == 0))(lambda: to_dp(0, mate, 0).start())
                pl.when(end & (s == 1))(lambda: to_dp(1, mate, 0).start())
            elif via_hub:

                @pl.when(end)
                def _():
                    to_dp(1, mate, 0).start()
                    to_dp(0, mate, 0).start()

        def side_weights():
            if by_side:

                @pl.when(end & (s == 1))
                def _():
                    to_side().wait_recv()
                    from_side().start()
                    to_dp(0, mate, 0).start()

        def send_weights(which):
            if via_hub:
                turn = [jnp.where(end, cross[0], mate), jnp.where(end, cross[1], cross[0]), jnp.where(end, mate, cross[1])]
                for k, p in enumerate(turn):
                    w_tx[p, which] = weight_grad(which, tile(p, share))

                    @pl.when(end)
                    def _():
                        for c in to_hub(which, 0) if k == 0 else to_hub(1, 1) + to_hub(0, 1) if k + which == 1 else []:
                            c.start()

                    if k == 0:

                        @pl.when(inner)
                        def _():
                            to_dp(which, mate, 0).start()

                if by_side and which == 1:

                    @pl.when(end & (s == 0))
                    def _():
                        to_side().start()

                w_tx[d, which] = weight_grad(which, tile(d, share))
            else:
                grad = weight_grad(which, pl.ds(0, feats))
                for p in range(n_dp):
                    w_tx[p, which] = grad[p * share : (p + 1) * share, :]
                for p in far:
                    to_dp(which, p, d).start()

        def pass_on(which, k, h):
            if via_hub:

                @pl.when(inner)
                def _():
                    to_hub(which, k)[h].wait_recv()
                    both = w_tx[cross[k], which, halves[h], :].astype(F32) + w_via[which, k, halves[h], :].astype(F32)
                    w_tx[cross[k], which, halves[h], :] = both.astype(BF16)
                    to_cross(which, k, h).start()

        send_weights(1)

        @pl.loop(0, n_mp)
        def _(r):
            back = dot_nn(g_all[r], wo_all[m])
            pre_all[tile(r, quarter), :] = (back * slope_all[tile(r, quarter), :]).astype(BF16)

        pass_on(1, 0, 0)
        send_weights(0)
        last_weights()
        pass_on(1, 0, 1)
        for h in range(2):
            pass_on(0, 0, h)
        in_spread = Spread(slab, in_s, in_a, in_i)

        @pl.when(s != 0)
        def _():
            copy(g_new.at[:, 0:width], slab(m), ix_s, ix_r, {"section": 0}).wait_recv()

        in_spread.start()

        total = i_tx[d].astype(F32)
        wait_all(i_rx.at[pl.ds(0, n_dp - 1)], im_r)
        for p in near:
            total = total + i_rx[p].astype(F32)
        unit, length = unit_rows(image[mine_half, :])
        image_out[mine_half, :] = unit_backward(unit, length, mult * total).astype(BF16)
        for t in others(s, n_sec):
            copy(image_out.at[mine_half, :], image_out.at[mine_half, :], io_s, io_r, {"section": t}).start()

        side_weights()
        for which in (1, 0):
            for h in range(2):
                pass_on(which, 1, h)
        in_spread.relay()
        in_spread.finish()

        wait_all(image_out.at[pl.ds(0, (n_sec - 1) * half), :], io_r)

        wait_all(cols.at[pl.ds(0, (n_dp - 1) * half), :], gat_s)
        wait_all(col_rx.at[pl.ds(0, n_dp - 1)], cs_s)
        wait_all(row_rx.at[pl.ds(0, n_sec * n_mp - 1)], rs_s)
        wait_all(wi_all.at[pl.ds(0, n_mp - 1)], wi_s)
        wait_all(wo_all.at[pl.ds(0, n_mp - 1)], wo_s)
        if cores > 1:
            wait_all(a_tx, a_s)
        if chips > 1:
            wait_all(b_tx.at[pl.ds(0, chips - 1)], b_s)
        wait_all(g_all.at[pl.ds(0, n_mp - 1)], g_s)
        wait_all(i_tx.at[pl.ds(0, n_dp - 1)], im_s)
        wait_all(input_out.at[pl.ds(0, (n_mp - 1) * quarter), :], in_s)
        wait_all(image_out.at[pl.ds(0, (n_sec - 1) * half), :], io_s)

        @pl.when(s != last)
        def _():
            wait_all(c_tx, c_s)

        @pl.when(s > 0)
        def _():
            wait_all(g_new, x_s)

        @pl.when(s == 0)
        def _():
            wait_all(g_new.at[:, pl.ds(0, (n_sec - 1) * width)], ix_s)

        for which, out in ((1, second_out), (0, first_out)):
            out[...] = w_tx[d, which].astype(F32)

            for p in [0] if via_hub else near:
                copy(w_rx.at[p, which], w_rx.at[p, which], w_s, w_r.at[which, p], {"dp": mate}).wait_recv()
                out[...] += w_rx[p, which].astype(F32)
            for h, at in enumerate(halves if via_hub else []):
                to_cross(which, 0, h).wait_recv()
                out[at, :] += w_rx[1, which, at, :].astype(F32)
        wait_all(w_tx.at[pl.ds(0, n_dp - 1)], w_s)
        if by_side:
            pl.when(end & (s == 1))(lambda: wait_all(w_side, sd_s))

    return kernel


def store(image, inputs, first, second, image_out, input_out, first_out, second_out, sems):
    copies = [
        pltpu.make_async_copy(image, image_out, sems.at[0]),
        pltpu.make_async_copy(inputs, input_out, sems.at[1]),
        pltpu.make_async_copy(first, first_out.at[0], sems.at[2]),
        pltpu.make_async_copy(second, second_out.at[0], sems.at[3]),
    ]
    for c in copies:
        c.start()
    for c in copies:
        c.wait()


def solution(mesh):
    n_sec, n_dp, n_mp = mesh.shape["section"], mesh.shape["dp"], mesh.shape["mp"]

    def body(text, image, scale, hidden, w_in, w_out):
        rows, feats = text.shape
        own = image.shape[0]
        hid = w_in.shape[2]
        quarter, half, share = rows // n_mp, own // n_sec, feats // n_dp
        columns = half * n_dp
        cores = 2 if n_mp % 2 == 0 else 1
        chips = n_mp // cores
        away = max(chips - 1, 1)
        dma = pltpu.SemaphoreType.DMA
        vmem = pl.BlockSpec(memory_space=pltpu.VMEM)
        hbm = pl.BlockSpec(memory_space=pltpu.HBM)
        out = pl.pallas_call(
            make_kernel(n_sec, n_dp, n_mp),
            out_shape=(
                pltpu.VMEM((own, feats), BF16),
                pltpu.VMEM((rows, feats // n_sec), BF16),
                pltpu.VMEM((share, hid), F32),
                pltpu.VMEM((share, hid), F32),
            ),
            in_specs=[hbm, hbm, pl.BlockSpec(memory_space=pltpu.SMEM), hbm, hbm, hbm],
            out_specs=(vmem,) * 4,
            scratch_shapes=[
                pltpu.VMEM((rows, feats), BF16),
                pltpu.VMEM((own, feats), BF16),
                pltpu.VMEM((rows, feats), BF16),
                pltpu.VMEM((rows, feats), BF16),
                pltpu.VMEM((columns, feats), BF16),
                pltpu.VMEM((rows, columns), F32),
                pltpu.VMEM((rows, columns), BF16),
                pltpu.VMEM((rows, LANES), F32),
                pltpu.VMEM((rows, LANES), F32),
                pltpu.VMEM((n_mp, quarter, LANES), F32),
                pltpu.VMEM((2 * n_mp, quarter), F32),
                pltpu.VMEM((n_sec * n_mp, 2 * n_mp, quarter), F32),
                pltpu.VMEM((2 * n_dp, half), F32),
                pltpu.VMEM((n_dp, 2 * n_dp, half), F32),
                pltpu.VMEM((feats, hid), BF16),
                pltpu.VMEM((hid, feats), BF16),
                pltpu.VMEM((n_mp, hid, feats), BF16),
                pltpu.VMEM((n_mp, feats, hid), BF16),
                pltpu.VMEM((n_mp, quarter, hid), F32),
                pltpu.VMEM((rows, hid), F32),
                pltpu.VMEM((rows, hid), BF16),
                pltpu.VMEM((rows, hid), BF16),
                pltpu.VMEM((quarter // PIECES * GROUP, n_mp * hid), BF16),
                pltpu.VMEM((chips, quarter, feats), BF16),
                pltpu.VMEM((chips, quarter, feats), BF16),
                pltpu.VMEM((chips, quarter, feats), BF16),
                pltpu.VMEM((chips, quarter, feats), BF16),
                pltpu.VMEM((quarter, feats), BF16),
                pltpu.VMEM((n_sec, quarter, feats), BF16),
                pltpu.VMEM((quarter, feats), F32),
                pltpu.VMEM((n_mp, quarter, feats), BF16),
                pltpu.VMEM((quarter, feats), BF16),
                pltpu.VMEM((feats, hid), F32),
                pltpu.VMEM((n_dp, 2, share, hid), BF16),
                pltpu.VMEM((n_dp, 2, share, hid), BF16),
                pltpu.VMEM((2, 2, share, hid), BF16),
                pltpu.VMEM((share, hid), BF16),
                pltpu.VMEM((n_dp, half, feats), BF16),
                pltpu.VMEM((n_dp, half, feats), BF16),
                dma((5,)),
                dma, dma((n_dp,)),
                dma, dma,
                dma, dma,
                dma, dma((2, away)), dma((2, chips)),
                dma, dma((away,)), dma, dma((away,)), dma((away, 2)),
                dma, dma((chips,)),
                dma, dma((away, PIECES)),
                dma, dma((n_sec - 1, PIECES)),
                dma, dma((away, PIECES)), dma((chips, PIECES // GROUP)),
                dma, dma((PIECES,)),
                dma, dma((away,)), dma((chips,)),
                dma, dma,
                dma, dma((2, 3 if n_dp == 4 else n_dp)), dma((2, 2, 2)), dma, dma,
                dma, dma,
                dma, dma,
            ],
            compiler_params=pltpu.CompilerParams(
                collective_id=0, has_side_effects=True, vmem_limit_bytes=50000000
            ),
        )(*(pltpu.with_memory_space_constraint(x, pltpu.HBM) for x in (text, image)), scale,
          *(pltpu.with_memory_space_constraint(x[0], pltpu.HBM) for x in (hidden, w_in, w_out)))
        return tuple(
            pl.pallas_call(
                store,
                out_shape=(
                    jax.ShapeDtypeStruct((own, feats), BF16),
                    jax.ShapeDtypeStruct((rows, feats // n_sec), BF16),
                    jax.ShapeDtypeStruct((1, share, hid), F32),
                    jax.ShapeDtypeStruct((1, share, hid), F32),
                ),
                in_specs=[vmem] * 4,
                out_specs=(hbm,) * 4,
                scratch_shapes=[dma((4,))],
                compiler_params=pltpu.CompilerParams(has_side_effects=True),
            )(*(pltpu.with_memory_space_constraint(x, pltpu.VMEM) for x in out))
        )

    return jax.shard_map(
        body,
        mesh=mesh,
        in_specs=(
            P("dp", None),
            P(("dp", "mp"), None),
            P(),
            P("section", "dp", None),
            P("section", None, "mp"),
            P("section", "mp", None),
        ),
        out_specs=(
            P(("dp", "mp"), None),
            P("dp", "section"),
            P("section", "dp", "mp"),
            P("section", "dp", "mp"),
        ),
        check_vma=False,
    )
```

```python
import jax
import jax.numpy as jnp
from jax import lax
from jax.experimental import pallas as pl
from jax.experimental.pallas import tpu as pltpu
from jax.sharding import PartitionSpec as P

MESH = pl.DeviceIdType.MESH
F32 = jnp.float32
BF16 = jnp.bfloat16
GELU = 1.702
LANES = 128
PIECES = 8
GROUP = 2


def unit_rows(values):
    wide = values.astype(F32)
    length = jnp.sqrt(jnp.sum(wide * wide, axis=1, keepdims=True) + 1.0)
    return (wide / length, length)


def unit_backward(unit, length, grad_unit):
    return (grad_unit - unit * jnp.sum(unit * grad_unit, axis=1, keepdims=True)) / length


def dot_nn(a, b):
    return lax.dot_general(a, b, (((1,), (0,)), ((), ())), preferred_element_type=F32)


def dot_nt(a, b):
    return lax.dot_general(a, b, (((1,), (1,)), ((), ())), preferred_element_type=F32)


def dot_tn(a, b):
    return lax.dot_general(a, b, (((0,), (0,)), ((), ())), preferred_element_type=F32)


def tile(index, size):
    return pl.ds(pl.multiple_of(index * size, size), size)


def pick(index, values):
    out = 0
    for k, v in enumerate(values):
        out = out + jnp.where(index == k, v, 0)
    return out


def nearest(count):
    return [sorted((p for p in range(count) if p != i), key=lambda p: (abs(p - i), p)) for i in range(count)]


def make_kernel(n_sec, n_dp, n_mp):
    cores = 2 if n_mp % 2 == 0 else 1
    chips = n_mp // cores

    def kernel(
        text_in, image_in, scale_ref, hidden_in, w_in, w_out,
        image_out, input_out, first_out, second_out,
        text, image, hidden,
        text_low, cols, scores, sgrad, row_max, row_sum, row_lse, row_st, row_rx, col_st, col_rx,
        raw_in, raw_out, wi_all, wo_all, slope_own, slope_all, act_all, pre_all, grad_own,
        a_tx, a_rx, b_tx, b_rx, c_tx, c_rx, t_acc, g_all, g_new,
        w_acc, w_tx, w_rx, w_via, w_side, i_tx, i_rx,
        ld, gat_s, gat_r, cs_s, cs_r, rs_s, rs_r, wi_s, wi_a, wi_i,
        wo_s, yo_r, so_r, zo_r, fo_r, a_s, a_r, b_s, b_r, c_s, c_r, g_s, ga_r, gi_r, x_s,
        in_s, in_a, in_i, ix_s, ix_r, w_s, w_r, v_r, sd_s, sd_r, im_s, im_r, io_s, io_r,
    ):
        s = lax.axis_index("section")
        d = lax.axis_index("dp")
        m = lax.axis_index("mp")
        last = n_sec - 1
        rows, feats = text.shape
        own = image.shape[0]
        half = own // n_sec
        quarter = rows // n_mp
        piece = quarter // PIECES
        hid = slope_all.shape[1]
        share = feats // n_dp
        width = feats // n_sec
        mult = scale_ref[0]
        core = lax.rem(m, cores)
        chip = m // cores

        def copy(src, dst, send, recv, where):
            return pltpu.make_async_remote_copy(
                src_ref=src, dst_ref=dst, send_sem=send, recv_sem=recv,
                device_id=where, device_id_type=MESH,
            )

        def wait_all(ref, sem):
            pltpu.make_async_copy(ref, ref, sem).wait()

        def others(mine, count):
            return [lax.rem(mine + k, count) for k in range(1, count)]

        def sources(mine, count):
            return [lax.rem(mine + count - k, count) for k in range(1, count)]

        order = nearest(n_dp)
        near = [pick(d, [order[i][k] for i in range(n_dp)]) for k in range(n_dp - 1)]
        far = near[::-1]

        barrier = pltpu.get_barrier_semaphore()
        plane = [(t, p) for t in [s] + others(s, n_sec) for p in [m] + others(m, n_mp)][1:]
        for t, p in plane:
            pl.semaphore_signal(barrier, inc=1, device_id={"section": t, "mp": p}, device_id_type=MESH)
        for p in near:
            pl.semaphore_signal(barrier, inc=1, device_id={"dp": p}, device_id_type=MESH)
        via_hub = n_dp == 4
        by_side = via_hub and n_sec == 2
        mate = d + 1 - 2 * lax.rem(d, 2)
        if by_side:
            pl.semaphore_signal(barrier, inc=1, device_id={"section": 1 - s, "dp": mate}, device_id_type=MESH)

        loads = [
            pltpu.make_async_copy(image_in, image, ld.at[0]),
            pltpu.make_async_copy(w_in, raw_in, ld.at[1]),
            pltpu.make_async_copy(w_out, raw_out, ld.at[2]),
            pltpu.make_async_copy(text_in, text, ld.at[3]),
            pltpu.make_async_copy(hidden_in, hidden, ld.at[4]),
        ]
        for c in loads:
            c.start()

        mine_half = tile(s, half)
        loads[0].wait()
        own_unit, _ = unit_rows(image[mine_half, :])
        cols[tile(d, half), :] = own_unit.astype(BF16)
        pl.semaphore_wait(barrier, len(plane) + n_dp - 1 + (1 if by_side else 0))

        for p in far:
            copy(cols.at[tile(d, half), :], cols.at[tile(d, half), :], gat_s, gat_r.at[d], {"dp": p}).start()

        class Spread:
            def __init__(self, slot, send, across, inside):
                self.slot, self.send, self.across, self.inside = slot, send, across, inside

            def push(self, index, recv, to):
                copy(self.slot(index), self.slot(index), self.send, recv, {"mp": to}).start()

            def start(self):
                for k, q in enumerate(others(chip, chips)):
                    self.push(m, self.across.at[k], q * cores + core)
                for e in others(core, cores):
                    self.push(m, self.inside.at[chip], chip * cores + e)

            def relay(self):
                for k, q in enumerate(sources(chip, chips)):
                    index = q * cores + core
                    copy(self.slot(index), self.slot(index), self.send, self.across.at[k], {"mp": index}).wait_recv()
                    for e in others(core, cores):
                        self.push(index, self.inside.at[q], chip * cores + e)

            def finish(self):
                for e in sources(core, cores):
                    for q in range(chips):
                        slot = self.slot(q * cores + e)
                        copy(slot, slot, self.send, self.inside.at[q], {"mp": chip * cores + e}).wait_recv()

        pairs = 2 if n_dp % 2 == 0 else 1
        side = lax.rem(d, pairs)
        depth = feats // pairs

        def wo_part(index, k):
            return wo_all.at[index, tile(k, depth), :]

        loads[2].wait()
        wo_all[m] = raw_out[...].T
        def wo_push(ref, recv, to):
            copy(ref, ref, wo_s, recv, to).start()

        for k, q in enumerate(others(chip, chips)):
            wo_push(wo_part(m, side), yo_r.at[k], {"mp": q * cores + core})
        for e in others(core, cores):
            wo_push(wo_all.at[m], so_r, {"mp": chip * cores + e})

        loads[1].wait()
        wi_all[m] = raw_in[...].T

        def wi_spread_of(k):
            return Spread(lambda j: wi_all.at[j, pl.ds(k * (hid // 2), hid // 2), :], wi_s, wi_a.at[k], wi_i.at[k])

        wi_spread = [wi_spread_of(k) for k in range(2)]
        wi_spread[0].start()

        def wo_across():
            for k, q in enumerate(sources(chip, chips)):
                index = q * cores + core
                at = wo_part(index, side)
                copy(at, at, wo_s, yo_r.at[k], {"mp": index}).wait_recv()
                if pairs == 2:
                    wo_push(at, zo_r.at[k], {"dp": d + 1 - 2 * side})
                for e in others(core, cores):
                    wo_push(at, fo_r.at[k, 0], {"mp": chip * cores + e})

        def wo_along():
            for k, q in enumerate(sources(chip, chips)):
                at = wo_part(q * cores + core, 1 - side)
                if pairs == 2:
                    copy(at, at, wo_s, zo_r.at[k], {"dp": d + 1 - 2 * side}).wait_recv()
                    for e in others(core, cores):
                        wo_push(at, fo_r.at[k, 1], {"mp": chip * cores + e})

        def wo_finish():
            for e in sources(core, cores):
                to = {"mp": chip * cores + e}
                own_block = wo_all.at[chip * cores + e]
                copy(own_block, own_block, wo_s, so_r, to).wait_recv()
                for i, q in enumerate(sources(chip, chips)):
                    for k in range(pairs):
                        at = wo_part(q * cores + e, side if k == 0 else 1 - side)
                        copy(at, at, wo_s, fo_r.at[i, k], to).wait_recv()

        loads[3].wait()

        @pl.loop(0, n_mp)
        def _(r):
            unit, _ = unit_rows(text[tile(r, quarter), :])
            text_low[tile(r, quarter), :] = unit.astype(BF16)

        row_max[...] = jnp.full(row_max.shape, -1e30, F32)
        row_sum[...] = jnp.zeros(row_sum.shape, F32)

        def block_scores(p):
            block = cols[tile(p, half), :]
            peak = jnp.full((1, half), -1e30, F32)
            for r in range(n_mp):
                part = pl.ds(r * quarter, quarter)
                value = mult * dot_nt(text_low[part, :], block)
                scores[part, tile(p, half)] = value
                peak = jnp.maximum(peak, jnp.max(value, axis=0, keepdims=True))
            acc = jnp.zeros((1, half), F32)
            for r in range(n_mp):
                value = scores[pl.ds(r * quarter, quarter), tile(p, half)]
                acc = acc + jnp.sum(jnp.exp(value - peak), axis=0, keepdims=True)
            col_st[pl.ds(p, 1), :] = peak
            col_st[pl.ds(n_dp + p, 1), :] = acc

        def block_rows(p):
            for r in range(n_mp):
                part = pl.ds(r * quarter, quarter)
                old = row_max[part, :]
                best = old
                value = [scores[part, pl.ds(pl.multiple_of(p * half + k, LANES), LANES)] for k in range(0, half, LANES)]
                for v in value:
                    best = jnp.maximum(best, v)
                acc = row_sum[part, :] * jnp.exp(old - best)
                for v in value:
                    acc = acc + jnp.exp(v - best)
                row_max[part, :] = best
                row_sum[part, :] = acc

        block_scores(d)
        block_rows(d)

        def gelu_terms(pre):
            sigm = 1.0 / (1.0 + jnp.exp(-GELU * pre))
            return pre * sigm, sigm + GELU * pre * sigm * (1.0 - sigm)

        loads[4].wait()

        @pl.loop(0, n_mp)
        def _(r):
            act, slope = gelu_terms(dot_nn(hidden[tile(r, quarter), :], raw_in[...]))
            act_all[tile(r, quarter), :] = act.astype(BF16)
            slope_all[tile(r, quarter), :] = slope

        @pl.loop(0, n_dp - 1)
        def _(k):
            p = near[0]
            for i in range(1, n_dp - 1):
                p = jnp.where(k == i, near[i], p)
            copy(cols.at[tile(p, half), :], cols.at[tile(p, half), :], gat_s, gat_r.at[p], {"dp": p}).wait_recv()
            block_scores(p)

            @pl.when(k < n_dp - 2)
            def _():
                block_rows(p)

        col_rx[d] = col_st[...]
        for p in far:
            copy(col_st, col_rx.at[d], cs_s, cs_r, {"dp": p}).start()

        wo_across()
        block_rows(far[0])

        for r in range(n_mp):
            part = pl.ds(r * quarter, quarter)
            peak = jnp.max(row_max[part, :], axis=1, keepdims=True)
            acc = jnp.sum(row_sum[part, :] * jnp.exp(row_max[part, :] - peak), axis=1, keepdims=True)
            wide_peak = jnp.broadcast_to(peak, (quarter, LANES)).T
            wide_sum = jnp.broadcast_to(acc, (quarter, LANES)).T
            row_st[r : r + 1, :] = wide_peak[0:1, :]
            row_st[n_mp + r : n_mp + r + 1, :] = wide_sum[0:1, :]

        here = s * n_mp + m
        row_rx[here] = row_st[...]
        for k, (t, p) in enumerate(plane):
            copy(row_st, row_rx.at[here], rs_s, rs_r, {"section": t, "mp": p}).start()

        wi_spread[1].start()
        wi_spread[0].relay()

        def merge(rx, count, n):
            peak = rx[0, 0:n, :]
            for k in range(1, count):
                peak = jnp.maximum(peak, rx[k, 0:n, :])
            acc = jnp.zeros(peak.shape, F32)
            for k in range(count):
                acc = acc + rx[k, n : 2 * n, :] * jnp.exp(rx[k, 0:n, :] - peak)
            return peak + jnp.log(acc)

        wait_all(row_rx.at[pl.ds(0, n_sec * n_mp - 1)], rs_r)
        merged = merge(row_rx, n_sec * n_mp, n_mp)
        for r in range(n_mp):
            row_lse[r] = jnp.broadcast_to(merged[r : r + 1, :], (LANES, quarter)).T

        wait_all(col_rx.at[pl.ds(0, n_dp - 1)], cs_r)
        col_lse = merge(col_rx, n_dp, n_dp)

        def score_rows(r):
            line = row_lse[r]
            for p in range(n_dp):
                for k in range(0, half, LANES):
                    at = pl.ds(p * half + k, LANES)
                    value = scores[tile(r, quarter), at]
                    both = jnp.exp(value - line) + jnp.exp(value - col_lse[p : p + 1, k : k + LANES])
                    sgrad[tile(r, quarter), at] = (0.5 * both).astype(BF16)

        def score_diagonal():
            line = row_lse[m]
            text_id = lax.broadcasted_iota(jnp.int32, (quarter, LANES), 0)
            lse = col_lse[0:1, :]
            for p in range(1, n_dp):
                lse = jnp.where(d == p, col_lse[p : p + 1, :], lse)
            for k in range(0, half, LANES):
                at = pl.ds(pl.multiple_of(d * half + k, LANES), LANES)
                value = scores[tile(m, quarter), at]
                both = jnp.exp(value - line) + jnp.exp(value - lse[:, k : k + LANES])
                image_id = lax.broadcasted_iota(jnp.int32, (quarter, LANES), 1) + (s * half + k)
                out = 0.5 * both - jnp.where(text_id == image_id, 1.0, 0.0)
                sgrad[tile(m, quarter), at] = out.astype(BF16)

        def text_part(r):
            return dot_nn(sgrad[tile(r, quarter), :], cols[...])

        def rows_of(k):
            return tile(k, piece)

        def for_sibling(q):
            for e in others(core, cores):
                r = q * cores + e
                score_rows(r)
                a_tx[q] = text_part(r).astype(BF16)
                copy(a_tx.at[q], a_rx.at[q], a_s, a_r.at[q], {"mp": chip * cores + e}).start()

        def from_sibling(q):
            for e in others(core, cores):
                copy(a_tx.at[q], a_rx.at[q], a_s, a_r.at[q], {"mp": chip * cores + e}).wait_recv()
                t_acc[...] += a_rx[q].astype(F32)

        for i, q in enumerate(others(chip, chips)):
            for_sibling(q)
            score_rows(q * cores + core)
            t_acc[...] = text_part(q * cores + core)
            from_sibling(q)
            b_tx[q] = t_acc[...].astype(BF16)
            for k in range(PIECES):
                copy(b_tx.at[q, rows_of(k), :], b_rx.at[i, rows_of(k), :], b_s, b_r.at[i, k],
                     {"mp": q * cores + core}).start()
        for_sibling(chip)
        score_rows(m)
        score_diagonal()
        t_acc[...] = text_part(m)

        def image_part(p):
            return dot_tn(sgrad[:, tile(p, half)], text_low[...])

        for p in far:
            i_tx[p] = image_part(p).astype(BF16)
            copy(i_tx.at[p], i_rx.at[d], im_s, im_r, {"dp": p}).start()
        i_tx[d] = image_part(d).astype(BF16)

        from_sibling(chip)
        mine = tile(m, quarter)
        wi_spread[1].relay()
        wo_along()

        def gather_sum(k):
            total = t_acc[rows_of(k), :]
            for i, q in enumerate(sources(chip, chips)):
                copy(b_tx.at[q, rows_of(k), :], b_rx.at[i, rows_of(k), :], b_s, b_r.at[i, k],
                     {"mp": q * cores + core}).wait_recv()
                total = total + b_rx[i, rows_of(k), :].astype(F32)
            return total

        def to_last(k):
            return copy(c_tx.at[rows_of(k), :], c_rx.at[s, rows_of(k), :], c_s, c_r.at[s, k],
                        {"section": last})

        def to_below(k):
            return copy(g_new.at[rows_of(k), :], g_all.at[m, rows_of(k), :], x_s, c_r.at[0, k],
                        {"section": s - 1})

        @pl.when(s != last)
        def _():
            @pl.loop(0, PIECES)
            def _(k):
                c_tx[rows_of(k), :] = gather_sum(k).astype(BF16)
                to_last(k).start()

        def own_slope(j):
            _, slope = gelu_terms(dot_nt(hidden[mine, :], wi_all[j]))
            slope_own[j] = slope

        own_slope(m)
        for spread in wi_spread:
            spread.finish()

        @pl.loop(1, n_mp)
        def _(k):
            own_slope(lax.rem(m + k, n_mp))

        wo_finish()

        def g_push(k, index, recv, to):
            slot = g_all.at[index, rows_of(k), :]
            copy(slot, slot, g_s, recv, {"mp": to}).start()

        @pl.loop(0, PIECES // GROUP)
        def _(i):
            @pl.loop(i * GROUP, (i + 1) * GROUP)
            def _(k):
                at = tile(m * PIECES + k, piece)

                @pl.when(s == last)
                def _():
                    total = gather_sum(k)
                    for t in range(last):
                        copy(c_tx.at[rows_of(k), :], c_rx.at[t, rows_of(k), :], c_s, c_r.at[t, k],
                             {"section": t}).wait_recv()
                        total = total + c_rx[t, rows_of(k), :].astype(F32)
                    unit, length = unit_rows(text[at, :])
                    g_all[m, rows_of(k), :] = unit_backward(unit, length, mult * total).astype(BF16)

                @pl.when(s != last)
                def _():
                    copy(g_new.at[rows_of(k), :], g_all.at[m, rows_of(k), :], x_s, c_r.at[0, k],
                         {"section": s + 1}).wait_recv()

                for j, q in enumerate(others(chip, chips)):
                    g_push(k, m, ga_r.at[j, k], q * cores + core)

            group = tile(i, GROUP * piece)
            for e in others(core, cores):
                slot = g_all.at[m, group, :]
                copy(slot, slot, g_s, gi_r.at[chip, i], {"mp": chip * cores + e}).start()
            g = g_all[m, group, :]
            for j in range(n_mp):
                back = dot_nn(g, wo_all[j])
                grad_own[:, j * hid : (j + 1) * hid] = (back * slope_own[j, group, :]).astype(BF16)
            acc = dot_nn(grad_own[...], wi_all[...].reshape(n_mp * hid, feats))
            g_new[group, :] = (g.astype(F32) + acc).astype(BF16)

            @pl.when(s > 0)
            def _():
                for k in range(GROUP):
                    to_below(i * GROUP + k).start()

        groups = PIECES // GROUP

        def group_of(i):
            return pl.ds(i * GROUP * piece, GROUP * piece)

        def relay_group(i):
            for j, q in enumerate(sources(chip, chips)):
                index = q * cores + core
                for k in range(i * GROUP, (i + 1) * GROUP):
                    slot = g_all.at[index, rows_of(k), :]
                    copy(slot, slot, g_s, ga_r.at[j, k], {"mp": index}).wait_recv()
                slot = g_all.at[index, group_of(i), :]
                for e in others(core, cores):
                    copy(slot, slot, g_s, gi_r.at[q, i], {"mp": chip * cores + e}).start()

        def sibling_groups(q):
            for i in range(groups):
                for e in sources(core, cores):
                    slot = g_all.at[q * cores + e, group_of(i), :]
                    copy(slot, slot, g_s, gi_r.at[q, i], {"mp": chip * cores + e}).wait_recv()

        def chip_grad(q, at):
            left = g_all[pl.ds(q * cores, cores), :, at]
            return dot_tn(left.reshape(cores * quarter, left.shape[2]), act_all[tile(q, cores * quarter), :])

        for i in range(groups - 2):
            relay_group(i)
        sibling_groups(chip)
        relay_group(groups - 2)
        w_acc[...] = chip_grad(chip, pl.ds(0, feats))
        relay_group(groups - 1)

        def slab(k):
            return input_out.at[tile(k, quarter), :]

        def final(t):
            return copy(g_new.at[:, t * width : (t + 1) * width], slab(m), ix_s, ix_r,
                        {"section": t})

        @pl.when(s == 0)
        def _():
            for t in range(1, n_sec):
                final(t).start()
            input_out[mine, :] = g_new[:, 0:width]

        for q in sources(chip, chips):
            sibling_groups(q)

        low = d < n_dp // 2
        end = (d == 0) | (d == n_dp - 1)
        inner = jnp.logical_not(end)
        cross = [jnp.where(low, n_dp - 1, 0), jnp.where(low, n_dp - 2, 1)]

        def weight_grad(which, at):
            if which == 1:
                total = w_acc[at, :]
                for q in sources(chip, chips):
                    total = total + chip_grad(q, at)
                return total.astype(BF16)
            return dot_tn(hidden[:, at], pre_all[...]).astype(BF16)

        halves = [pl.ds(h * (share // 2), share // 2) for h in range(2)]

        def to_dp(which, p, slot):
            return copy(w_tx.at[p, which], w_rx.at[slot, which], w_s, w_r.at[which, slot], {"dp": p})

        def to_hub(which, k):
            return [
                copy(w_tx.at[cross[k], which, at, :], w_via.at[which, k, at, :], w_s, v_r.at[which, k, h], {"dp": mate})
                for h, at in enumerate(halves)
            ]

        def to_cross(which, k, h):
            return copy(w_tx.at[cross[k], which, halves[h], :], w_rx.at[1, which, halves[h], :], w_s,
                        w_r.at[which, 1 + h], {"dp": cross[k]})

        def to_side():
            return copy(w_tx.at[mate, 1], w_side, w_s, sd_r, {"section": 1})

        def from_side():
            return copy(w_side, w_rx.at[0, 1], sd_s, w_r.at[1, 0], {"section": 0, "dp": mate})

        def last_weights():
            if by_side:
                pl.when(end & (s == 0))(lambda: to_dp(0, mate, 0).start())
                pl.when(end & (s == 1))(lambda: to_dp(1, mate, 0).start())
            elif via_hub:

                @pl.when(end)
                def _():
                    to_dp(1, mate, 0).start()
                    to_dp(0, mate, 0).start()

        def side_weights():
            if by_side:

                @pl.when(end & (s == 1))
                def _():
                    to_side().wait_recv()
                    from_side().start()
                    to_dp(0, mate, 0).start()

        def send_weights(which):
            if via_hub:
                turn = [jnp.where(end, cross[0], mate), jnp.where(end, cross[1], cross[0]), jnp.where(end, mate, cross[1])]
                for k, p in enumerate(turn):
                    w_tx[p, which] = weight_grad(which, tile(p, share))

                    @pl.when(end)
                    def _():
                        for c in to_hub(which, 0) if k == 0 else to_hub(1, 1) + to_hub(0, 1) if k + which == 1 else []:
                            c.start()

                    if k == 0:

                        @pl.when(inner)
                        def _():
                            to_dp(which, mate, 0).start()

                if by_side and which == 1:

                    @pl.when(end & (s == 0))
                    def _():
                        to_side().start()

                w_tx[d, which] = weight_grad(which, tile(d, share))
            else:
                grad = weight_grad(which, pl.ds(0, feats))
                for p in range(n_dp):
                    w_tx[p, which] = grad[p * share : (p + 1) * share, :]
                for p in far:
                    to_dp(which, p, d).start()

        def pass_on(which, k, h):
            if via_hub:

                @pl.when(inner)
                def _():
                    to_hub(which, k)[h].wait_recv()
                    both = w_tx[cross[k], which, halves[h], :].astype(F32) + w_via[which, k, halves[h], :].astype(F32)
                    w_tx[cross[k], which, halves[h], :] = both.astype(BF16)
                    to_cross(which, k, h).start()

        send_weights(1)

        @pl.loop(0, n_mp)
        def _(r):
            back = dot_nn(g_all[r], wo_all[m])
            pre_all[tile(r, quarter), :] = (back * slope_all[tile(r, quarter), :]).astype(BF16)

        pass_on(1, 0, 0)
        send_weights(0)
        last_weights()
        pass_on(1, 0, 1)
        for h in range(2):
            pass_on(0, 0, h)
        in_spread = Spread(slab, in_s, in_a, in_i)

        @pl.when(s != 0)
        def _():
            copy(g_new.at[:, 0:width], slab(m), ix_s, ix_r, {"section": 0}).wait_recv()

        in_spread.start()

        total = i_tx[d].astype(F32)
        wait_all(i_rx.at[pl.ds(0, n_dp - 1)], im_r)
        for p in near:
            total = total + i_rx[p].astype(F32)
        unit, length = unit_rows(image[mine_half, :])
        image_out[mine_half, :] = unit_backward(unit, length, mult * total).astype(BF16)
        for t in others(s, n_sec):
            copy(image_out.at[mine_half, :], image_out.at[mine_half, :], io_s, io_r, {"section": t}).start()

        side_weights()
        for which in (1, 0):
            for h in range(2):
                pass_on(which, 1, h)
        in_spread.relay()
        in_spread.finish()

        wait_all(image_out.at[pl.ds(0, (n_sec - 1) * half), :], io_r)

        wait_all(cols.at[pl.ds(0, (n_dp - 1) * half), :], gat_s)
        wait_all(col_rx.at[pl.ds(0, n_dp - 1)], cs_s)
        wait_all(row_rx.at[pl.ds(0, n_sec * n_mp - 1)], rs_s)
        wait_all(wi_all.at[pl.ds(0, n_mp - 1)], wi_s)
        wait_all(wo_all.at[pl.ds(0, n_mp - 1)], wo_s)
        if cores > 1:
            wait_all(a_tx, a_s)
        if chips > 1:
            wait_all(b_tx.at[pl.ds(0, chips - 1)], b_s)
        wait_all(g_all.at[pl.ds(0, n_mp - 1)], g_s)
        wait_all(i_tx.at[pl.ds(0, n_dp - 1)], im_s)
        wait_all(input_out.at[pl.ds(0, (n_mp - 1) * quarter), :], in_s)
        wait_all(image_out.at[pl.ds(0, (n_sec - 1) * half), :], io_s)

        @pl.when(s != last)
        def _():
            wait_all(c_tx, c_s)

        @pl.when(s > 0)
        def _():
            wait_all(g_new, x_s)

        @pl.when(s == 0)
        def _():
            wait_all(g_new.at[:, pl.ds(0, (n_sec - 1) * width)], ix_s)

        for which, out in ((1, second_out), (0, first_out)):
            out[...] = w_tx[d, which].astype(F32)

            for p in [0] if via_hub else near:
                copy(w_rx.at[p, which], w_rx.at[p, which], w_s, w_r.at[which, p], {"dp": mate}).wait_recv()
                out[...] += w_rx[p, which].astype(F32)
            for h, at in enumerate(halves if via_hub else []):
                to_cross(which, 0, h).wait_recv()
                out[at, :] += w_rx[1, which, at, :].astype(F32)
        wait_all(w_tx.at[pl.ds(0, n_dp - 1)], w_s)
        if by_side:
            pl.when(end & (s == 1))(lambda: wait_all(w_side, sd_s))

    return kernel


def store(image, inputs, first, second, image_out, input_out, first_out, second_out, sems):
    copies = [
        pltpu.make_async_copy(image, image_out, sems.at[0]),
        pltpu.make_async_copy(inputs, input_out, sems.at[1]),
        pltpu.make_async_copy(first, first_out.at[0], sems.at[2]),
        pltpu.make_async_copy(second, second_out.at[0], sems.at[3]),
    ]
    for c in copies:
        c.start()
    for c in copies:
        c.wait()


def solution(mesh):
    n_sec, n_dp, n_mp = mesh.shape["section"], mesh.shape["dp"], mesh.shape["mp"]

    def body(text, image, scale, hidden, w_in, w_out):
        rows, feats = text.shape
        own = image.shape[0]
        hid = w_in.shape[2]
        quarter, half, share = rows // n_mp, own // n_sec, feats // n_dp
        columns = half * n_dp
        cores = 2 if n_mp % 2 == 0 else 1
        chips = n_mp // cores
        away = max(chips - 1, 1)
        dma = pltpu.SemaphoreType.DMA
        vmem = pl.BlockSpec(memory_space=pltpu.VMEM)
        hbm = pl.BlockSpec(memory_space=pltpu.HBM)
        out = pl.pallas_call(
            make_kernel(n_sec, n_dp, n_mp),
            out_shape=(
                pltpu.VMEM((own, feats), BF16),
                pltpu.VMEM((rows, feats // n_sec), BF16),
                pltpu.VMEM((share, hid), F32),
                pltpu.VMEM((share, hid), F32),
            ),
            in_specs=[hbm, hbm, pl.BlockSpec(memory_space=pltpu.SMEM), hbm, hbm, hbm],
            out_specs=(vmem,) * 4,
            scratch_shapes=[
                pltpu.VMEM((rows, feats), BF16),
                pltpu.VMEM((own, feats), BF16),
                pltpu.VMEM((rows, feats), BF16),
                pltpu.VMEM((rows, feats), BF16),
                pltpu.VMEM((columns, feats), BF16),
                pltpu.VMEM((rows, columns), F32),
                pltpu.VMEM((rows, columns), BF16),
                pltpu.VMEM((rows, LANES), F32),
                pltpu.VMEM((rows, LANES), F32),
                pltpu.VMEM((n_mp, quarter, LANES), F32),
                pltpu.VMEM((2 * n_mp, quarter), F32),
                pltpu.VMEM((n_sec * n_mp, 2 * n_mp, quarter), F32),
                pltpu.VMEM((2 * n_dp, half), F32),
                pltpu.VMEM((n_dp, 2 * n_dp, half), F32),
                pltpu.VMEM((feats, hid), BF16),
                pltpu.VMEM((hid, feats), BF16),
                pltpu.VMEM((n_mp, hid, feats), BF16),
                pltpu.VMEM((n_mp, feats, hid), BF16),
                pltpu.VMEM((n_mp, quarter, hid), F32),
                pltpu.VMEM((rows, hid), F32),
                pltpu.VMEM((rows, hid), BF16),
                pltpu.VMEM((rows, hid), BF16),
                pltpu.VMEM((quarter // PIECES * GROUP, n_mp * hid), BF16),
                pltpu.VMEM((chips, quarter, feats), BF16),
                pltpu.VMEM((chips, quarter, feats), BF16),
                pltpu.VMEM((chips, quarter, feats), BF16),
                pltpu.VMEM((chips, quarter, feats), BF16),
                pltpu.VMEM((quarter, feats), BF16),
                pltpu.VMEM((n_sec, quarter, feats), BF16),
                pltpu.VMEM((quarter, feats), F32),
                pltpu.VMEM((n_mp, quarter, feats), BF16),
                pltpu.VMEM((quarter, feats), BF16),
                pltpu.VMEM((feats, hid), F32),
                pltpu.VMEM((n_dp, 2, share, hid), BF16),
                pltpu.VMEM((n_dp, 2, share, hid), BF16),
                pltpu.VMEM((2, 2, share, hid), BF16),
                pltpu.VMEM((share, hid), BF16),
                pltpu.VMEM((n_dp, half, feats), BF16),
                pltpu.VMEM((n_dp, half, feats), BF16),
                dma((5,)),
                dma, dma((n_dp,)),
                dma, dma,
                dma, dma,
                dma, dma((2, away)), dma((2, chips)),
                dma, dma((away,)), dma, dma((away,)), dma((away, 2)),
                dma, dma((chips,)),
                dma, dma((away, PIECES)),
                dma, dma((n_sec - 1, PIECES)),
                dma, dma((away, PIECES)), dma((chips, PIECES // GROUP)),
                dma,
                dma, dma((away,)), dma((chips,)),
                dma, dma,
                dma, dma((2, 3 if n_dp == 4 else n_dp)), dma((2, 2, 2)), dma, dma,
                dma, dma,
                dma, dma,
            ],
            compiler_params=pltpu.CompilerParams(
                collective_id=0, has_side_effects=True, vmem_limit_bytes=50000000
            ),
        )(*(pltpu.with_memory_space_constraint(x, pltpu.HBM) for x in (text, image)), scale,
          *(pltpu.with_memory_space_constraint(x[0], pltpu.HBM) for x in (hidden, w_in, w_out)))
        return tuple(
            pl.pallas_call(
                store,
                out_shape=(
                    jax.ShapeDtypeStruct((own, feats), BF16),
                    jax.ShapeDtypeStruct((rows, feats // n_sec), BF16),
                    jax.ShapeDtypeStruct((1, share, hid), F32),
                    jax.ShapeDtypeStruct((1, share, hid), F32),
                ),
                in_specs=[vmem] * 4,
                out_specs=(hbm,) * 4,
                scratch_shapes=[dma((4,))],
                compiler_params=pltpu.CompilerParams(has_side_effects=True),
            )(*(pltpu.with_memory_space_constraint(x, pltpu.VMEM) for x in out))
        )

    return jax.shard_map(
        body,
        mesh=mesh,
        in_specs=(
            P("dp", None),
            P(("dp", "mp"), None),
            P(),
            P("section", "dp", None),
            P("section", None, "mp"),
            P("section", "mp", None),
        ),
        out_specs=(
            P(("dp", "mp"), None),
            P("dp", "section"),
            P("section", "dp", "mp"),
            P("section", "dp", "mp"),
        ),
        check_vma=False,
    )
```
